32 devices in a mesh: col: 16 (over z, y, x), lev: 2 (over core).
Axes of the slice: x: 2, y: 2, z: 4, core: 2. Of those that a mesh axis runs over, the one named last changes fastest.
Arguments:
- perturbations: float32 [80, 16, 16384], P(None, 'lev', 'col'), may hold values from -0.625 to 0.625
- gradient: float32 [32, 16, 16384], P(None, 'lev', 'col'), may hold values from -2 to 2
- horizontal: float32 [20, 16384], P(None, 'col'), may hold values from -50 to 50
- area: float32 [16384], P('col'), may hold values from 1 to 60
- vertical: float32 [20, 16], P(None, 'lev'), may hold values from -1.25 to 1.25
Outputs:
- increment: float32 [32, 16, 16384], P(None, 'lev', 'col')
- background: float32 [32], replicated
The draws below stay inside these ranges and needn't reach their ends.
All inputs are finite; a program needn't handle non-finite values.
Results may differ from the reference program's by a relative error of at most 0.0003.
Values sent between devices are 32-bit elements; how exact they have to be, the bound alone decides.
A program may use at most 128 MiB of HBM per device.

```python
import math
import jax
import jax.numpy as jnp
from jax import lax

MEMBERS = 80
VMODES = 20
HMODES = 20
VECTORS = 32
LEV = 16
COLS = 16384


def draw_area(key, part):
    position = jnp.arange(COLS).astype(jnp.float32)
    ramped = 1.0 + 2.0 * position / max(COLS - 1, 1)
    rough = jnp.exp(jax.random.uniform(key, (COLS,), jnp.float32, 0.0, math.log(10.0)))
    return ramped * rough


def draw_horizontal(key, part):
    first, second = jax.random.split(jax.random.fold_in(key, 17), 2)
    row_scale = jnp.exp(jax.random.uniform(first, (HMODES, 1), jnp.float32, 0.0, math.log(10.0)))
    column_values = jnp.clip(jax.random.normal(second, (HMODES, COLS), jnp.float32), -5.0, 5.0)
    return row_scale * column_values


def shard_levels(key, dims, cuts, least, top_value):
    def one(dim, blocks):
        draws = jax.random.uniform(jax.random.fold_in(jax.random.fold_in(key, 6), dim), (blocks,), jnp.float32, least / len(cuts), top_value / len(cuts))
        return jnp.repeat(jnp.exp(draws), dims[dim] // blocks).reshape((-1,) + (1,) * (len(dims) - dim - 1))

    factor_of = one(*cuts[0])
    for cut in cuts[1:]:
        factor_of = factor_of * one(*cut)
    return factor_of


def centred(key, extent, width, bound, shards=(), dtype=jnp.bfloat16):
    values = width * jax.random.normal(key, extent, jnp.float32)
    if shards:
        values = values * shard_levels(key, extent, shards, -0.22, 0.18)
    return jnp.clip(values, -bound, bound).astype(dtype)


def setup_inputs(seed: int = 0) -> dict:
    seeds = jax.random.split(jax.random.key(seed), 6)
    return {
        "perturbations": centred(seeds[0], (MEMBERS, LEV, COLS), MEMBERS ** -0.5, 0.625, ((1, 2), (2, 16)), jnp.float32),
        "gradient": centred(seeds[1], (VECTORS, LEV, COLS), (max(1, LEV * COLS // (VMODES * HMODES * MEMBERS))) ** -0.5, 2.0, ((1, 2), (2, 16)), jnp.float32),
        "horizontal": draw_horizontal(jax.random.fold_in(seeds[5], 71), 0),
        "area": draw_area(jax.random.fold_in(seeds[5], 71), 0),
        "vertical": centred(seeds[4], (VMODES, LEV), VMODES ** -0.5, 1.25, ((1, 2),), jnp.float32),
    }


TOP_PRECISION = lax.Precision.HIGHEST

def reference(perturbations, gradient, horizontal, area, vertical):
    area_sum = jnp.sum(area)
    mode_power = lax.optimization_barrier(jnp.sum(area[None, :] * horizontal * horizontal, axis=1))
    scaled_terms = horizontal / jnp.sqrt(HMODES * (mode_power / area_sum + 1e-06))[:, None]
    weight = area * (COLS / area_sum)

    def adjoint_level(level_index):
        level_index = level_index.astype(jnp.int32)
        ensemble_member_rows = lax.dynamic_index_in_dim(perturbations, level_index, 1, keepdims=False)
        gradient_rows = lax.dynamic_index_in_dim(gradient, level_index, 1, keepdims=False)
        mode_products = (gradient_rows * weight[None, :])[:, None, :] * scaled_terms[None, :, :]
        return jnp.einsum('kc,vbc->kvb', ensemble_member_rows, mode_products, precision=TOP_PRECISION)
    terms = lax.map(adjoint_level, jnp.arange(LEV).astype(jnp.int32))
    control = jnp.einsum('al,lkvb->vkab', vertical, terms, precision=TOP_PRECISION)
    lifted = jnp.einsum('al,vkab->lkvb', vertical, control, precision=TOP_PRECISION)

    def forward_level_map(level_index):
        level_index = level_index.astype(jnp.int32)
        ensemble_member_rows = lax.dynamic_index_in_dim(perturbations, level_index, 1, keepdims=False)
        level_lift = lax.dynamic_index_in_dim(lifted, level_index, 0, keepdims=False)
        member_spread = jnp.einsum('kvb,kc->vbc', level_lift, ensemble_member_rows, precision=TOP_PRECISION)
        return lax.optimization_barrier(jnp.sum(member_spread * scaled_terms[None, :, :], axis=1))
    by_level = lax.map(forward_level_map, jnp.arange(LEV).astype(jnp.int32))
    increment = jnp.transpose(by_level, (1, 0, 2))
    background = 0.5 * lax.optimization_barrier(jnp.sum(control * control, axis=(1, 2, 3)))
    return (increment, background)
```

```python
import functools

import jax
import jax.numpy as jnp
from jax import lax
from jax.experimental import pallas as pl
from jax.experimental.pallas import tpu as pltpu
from jax.sharding import PartitionSpec as P

LANES = 128
NT = (((1,), (1,)), ((), ()))
TN = (((0,), (0,)), ((), ()))
NN = (((1,), (0,)), ((), ()))
UNROLL = 2


def split(x):
    high = x.astype(jnp.bfloat16)
    low = (x - high.astype(jnp.float32)).astype(jnp.bfloat16)
    return high, low


def exact_dot(a, b, dims):
    return lax.dot_general(
        a, b, dims, precision=lax.Precision.HIGHEST, preferred_element_type=jnp.float32
    )


def kernel(
    sizes, n, pert_ref, grad_ref, hor_ref, area_ref, vert_ref, out_ref, bg_ref,
    halves, weighted, acc, terms, first_a, first_b, second, third, reduced, lifted,
    stat_ref, stats, verticals, sums, parts, weights, scaled,
    send_h, recv_h, send_g, recv_g, send_l, recv_l, send_p, recv_p,
    send_s, recv_s, send_b, recv_b, send_v, recv_v,
):
    members, levels, vectors, modes, columns = sizes
    group = LANES // vectors
    chunks = modes // group
    vmodes = vert_ref.shape[1]
    rows = terms.shape[4]
    tiles = rows // levels
    outer = n // 4
    used = members * levels
    me = lax.axis_index("col")
    lev = lax.axis_index("lev")
    other = 1 - lev
    x = lax.rem(me, 2)
    y = lax.rem(lax.div(me, 2), 2)
    h = lax.div(me, 4)
    not_x, not_y = 1 - x, 1 - y
    x_peer = (4 * h + 2 * y + not_x, lev)
    y_peer = (4 * h + 2 * not_y + x, lev)
    mesh_id = pl.DeviceIdType.MESH
    barrier = pltpu.get_barrier_semaphore()

    def greet(p, carry):
        pl.semaphore_signal(
            barrier, inc=1, device_id=(lax.rem(me + p, n), lev), device_id_type=mesh_id
        )
        return carry

    lax.fori_loop(1, n, greet, 0)
    pl.semaphore_signal(barrier, inc=1, device_id=(me, other), device_id_type=mesh_id)

    def remote(src, dst, send, recv, device):
        return pltpu.make_async_remote_copy(
            src_ref=src, dst_ref=dst, send_sem=send, recv_sem=recv,
            device_id=device, device_id_type=mesh_id,
        )

    def halfway(j):
        count = (tiles + 1 - j % 2) // 2 * levels
        return pl.ds(0, count), pl.ds(count, rows - count), count, rows - count

    def half_copy(j, i, src, dst, device):
        return remote(src, dst, send_h.at[j, i], recv_h.at[j, i], device)

    def one(j):
        a, b, na, nb = halfway(j)
        return (
            half_copy(j, 0, terms.at[j, :, :, not_x, a], first_a.at[j, :, :, pl.ds(0, na)], x_peer),
            half_copy(j, 1, terms.at[j, :, not_y, :, b], first_b.at[j, :, :, pl.ds(0, nb)], y_peer),
        )

    def two(j):
        a, b, na, nb = halfway(j)
        return (
            half_copy(j, 2, first_a.at[j, :, not_y, pl.ds(0, na)], second.at[j, :, a], y_peer),
            half_copy(j, 3, first_b.at[j, :, not_x, pl.ds(0, nb)], second.at[j, :, b], x_peer),
        )

    def outer_copy(j, p):
        there = lax.rem(h + p, outer)
        device = (4 * there + 2 * y + x, lev)
        return remote(
            second.at[j, there], third.at[j, p], send_g.at[j, p], recv_g.at[j, p], device
        )

    def pair_copy(j, slot):
        block = reduced.at[j, slot]
        return remote(block, block, send_p.at[j], recv_p.at[j], (me, other))

    def lifted_copy(j, p, slot):
        there = lax.rem(h + p, outer)
        device = (4 * there + 2 * y + x, lev)
        block = lifted.at[j, slot, y, x]
        return remote(block, block, send_l.at[j, p], recv_l.at[j, p], device)

    def three(j, yy, xx):
        a, b, _, _ = halfway(j)
        block_a = lifted.at[j, :, yy, x, a]
        block_b = lifted.at[j, :, y, xx, b]
        return (
            half_copy(j, 4, block_a, block_a, y_peer),
            half_copy(j, 5, block_b, block_b, x_peer),
        )

    def four(j, yy, xx):
        a, b, _, _ = halfway(j)
        block_a = lifted.at[j, :, :, xx, a]
        block_b = lifted.at[j, :, yy, :, b]
        return (
            half_copy(j, 6, block_a, block_a, x_peer),
            half_copy(j, 7, block_b, block_b, y_peer),
        )

    def stat_copy(p, slot):
        peer = lax.rem(me + p, n)
        return remote(stat_ref, stats.at[slot], send_s.at[p], recv_s.at[p], (peer, lev))

    def part_copy(p, slot):
        peer = lax.rem(me + p, n)
        block = parts.at[slot]
        return remote(block, block, send_b.at[p], recv_b.at[p], (peer, lev))

    def vert_copy(slot):
        block = verticals.at[slot]
        return remote(block, block, send_v.at[0], recv_v.at[0], (me, other))

    area = area_ref[...]
    power = jnp.sum(area * hor_ref[...] * hor_ref[...], axis=1, keepdims=True)
    lane = lax.broadcasted_iota(jnp.int32, (modes, LANES), 1)
    row = lax.broadcasted_iota(jnp.int32, (modes, LANES), 0)
    powers = jnp.sum(
        jnp.where(lane == row, jnp.broadcast_to(power, (modes, LANES)), 0.0),
        axis=0, keepdims=True,
    )
    total = jnp.broadcast_to(jnp.sum(area, axis=1, keepdims=True), (1, LANES))
    stat_row = jnp.where(lane[:1] == modes, total, powers)
    stat_ref[...] = jnp.broadcast_to(stat_row, stat_ref.shape)
    verticals[lev] = jnp.zeros(verticals.shape[1:], jnp.float32)
    verticals[lev, :, :vmodes] = vert_ref[...]
    if used < n * rows:
        for j in range(chunks):
            flat = terms.at[j].reshape(n * rows, LANES)
            flat[used:, :] = jnp.zeros((n * rows - used, LANES), jnp.float32)
    for l in range(levels):
        high, low = split(pert_ref[:, l, :])
        halves[l, :members] = high
        halves[l, members:] = low
        weighted[l] = grad_ref[:, l, :] * area

    def over_levels(step):
        def body(i, carry):
            for u in range(UNROLL):
                step(i * UNROLL + u)
            return carry

        lax.fori_loop(0, levels // UNROLL, body, 0)

    def adjoint(j):
        flat = terms.at[j].reshape(n * rows, LANES)

        def step(l):
            base = weighted[l]
            products = jnp.concatenate(
                [base * hor_ref[b : b + 1, :] for b in range(j * group, (j + 1) * group)],
                axis=0,
            )
            both = jnp.concatenate(split(products), axis=0)
            out = lax.dot_general(halves[l], both, NT, preferred_element_type=jnp.float32)
            flat[pl.ds(l, members, stride=levels), :] = out[:members, :LANES] + (
                out[members:, :LANES] + out[:members, LANES:]
            )

        over_levels(step)

    def start(copies):
        for copy in copies:
            copy.start()

    def send_one(j):
        start(one(j))

    def send_two(j):
        a, b, na, nb = halfway(j)
        one_a, one_b = one(j)
        two_a, two_b = two(j)
        one_a.wait_recv()

        def add_a(i, carry):
            first_a[j, i, not_y, :na] += terms[j, i, not_y, x, a]
            return carry

        lax.fori_loop(0, outer, add_a, 0)
        two_a.start()
        one_b.wait_recv()

        def add_b(i, carry):
            first_b[j, i, not_x, :nb] += terms[j, i, y, not_x, b]
            return carry

        lax.fori_loop(0, outer, add_b, 0)
        two_b.start()

    def add_second(j, there):
        a, b, na, nb = halfway(j)
        second[j, there, a] += terms[j, there, y, x, a] + first_a[j, there, y, :na]
        second[j, there, b] += terms[j, there, y, x, b] + first_b[j, there, x, :nb]

    def send_three(j):
        for copy in two(j):
            copy.wait_recv()

        def send_outer(p, carry):
            add_second(j, lax.rem(h + p, outer))
            outer_copy(j, p).start()
            return carry

        lax.fori_loop(1, outer, send_outer, 0)
        add_second(j, h)
        reduced[j, lev] = second[j, h]

    def send_pair(j):
        def take(p, carry):
            outer_copy(j, p).wait_recv()
            reduced[j, lev] += third[j, p]
            return carry

        lax.fori_loop(1, outer, take, 0)
        pair_copy(j, lev).start()

    def mix(j):
        pair_copy(j, other).wait_recv()

        def wide(index):
            block = reduced[j, index]
            return jnp.concatenate(
                [block[i * levels : (i + 1) * levels] for i in range(tiles)], axis=1
            )

        control = exact_dot(verticals[0][:, :vmodes], wide(0), TN) + exact_dot(
            verticals[1][:, :vmodes], wide(1), TN
        )
        raised = exact_dot(vert_ref[...], control, NN)
        square = jnp.zeros((1, LANES), jnp.float32)
        for i in range(tiles):
            lanes = slice(i * LANES, (i + 1) * LANES)
            lifted[j, h, y, x, i * levels : (i + 1) * levels, :] = raised[:, lanes]
            square = square + jnp.sum(
                control[:, lanes] * control[:, lanes], axis=0, keepdims=True
            )
        sums[j : j + 1, :] = square

        def start_lifted(p, carry):
            lifted_copy(j, p, h).start()
            return carry

        lax.fori_loop(1, outer, start_lifted, 0)

    def send_g2(j):
        def take_lifted(p, carry):
            lifted_copy(j, p, lax.rem(h + outer - p, outer)).wait_recv()
            return carry

        lax.fori_loop(1, outer, take_lifted, 0)
        start(three(j, y, x))

    def send_g3(j):
        three_a, three_b = three(j, not_y, not_x)
        four_a, four_b = four(j, y, x)
        three_a.wait_recv()
        four_a.start()
        three_b.wait_recv()
        four_b.start()

    def forward(j):
        for copy in four(j, not_y, not_x):
            copy.wait_recv()
        flat = lifted.at[j].reshape(n * rows, LANES)
        width = 256

        def step(l):
            high, low = split(flat[pl.ds(l, members, stride=levels), :])
            lhs = jnp.concatenate([high, high, low], axis=0)
            for c in range(0, columns, width):
                cols = slice(c, c + width)
                rhs = jnp.concatenate([halves[l, :, cols], halves[l, :members, cols]], axis=0)
                spread = lax.dot_general(lhs, rhs, TN, preferred_element_type=jnp.float32)
                value = None if j == 0 else acc[l, :, cols]
                for g in range(group):
                    b = j * group + g
                    term = spread[g * vectors : (g + 1) * vectors] * scaled[b : b + 1, cols]
                    value = term if value is None else value + term
                if j == chunks - 1:
                    out_ref[:, l, cols] = value
                else:
                    acc[l, :, cols] = value

        if j == chunks - 1:
            for l in range(levels):
                step(l)
        else:
            over_levels(step)

    def take_stats():
        stats[me] = stat_ref[...]

        def take(p, carry):
            stat_copy(p, lax.rem(me + n - p, n)).wait_recv()
            return carry

        lax.fori_loop(1, n, take, 0)
        stat = lax.fori_loop(
            0, n, lambda i, c: c + stats[i], jnp.zeros(stat_ref.shape, jnp.float32)
        )
        spread = jnp.broadcast_to(stat[:1], (modes, LANES))
        power = jnp.sum(jnp.where(lane == row, spread, 0.0), axis=1, keepdims=True)
        whole = jnp.sum(jnp.where(lane == modes, spread, 0.0), axis=1, keepdims=True)
        factor = 1.0 / jnp.sqrt(modes * (power / whole + 1e-06))
        scale = factor * (columns * n / whole)
        scaled[...] = hor_ref[...] * (factor * scale)
        placed = jnp.where(
            lax.div(lane, vectors) == lax.rem(row, group),
            jnp.broadcast_to(scale, lane.shape), 0.0,
        )
        for j in range(chunks):
            weights[j : j + 1, :] = jnp.sum(
                placed[j * group : (j + 1) * group], axis=0, keepdims=True
            )

    def send_parts():
        part = jnp.zeros((1, LANES), jnp.float32)
        for j in range(chunks):
            weight = weights[j : j + 1, :]
            part = part + sums[j : j + 1, :] * weight * weight
        parts[me] = jnp.broadcast_to(part, parts.shape[1:])

        def start_parts(p, carry):
            part_copy(p, me).start()
            return carry

        lax.fori_loop(1, n, start_parts, 0)

    def take_parts():
        def take(p, carry):
            part_copy(p, lax.rem(me + n - p, n)).wait_recv()
            return carry

        lax.fori_loop(1, n, take, 0)
        part = lax.fori_loop(
            0, n, lambda i, c: c + parts[i], jnp.zeros(parts.shape[1:], jnp.float32)
        )
        folded = part
        for g in range(1, group):
            folded = folded + pltpu.roll(part, g * vectors, 1)
        bg_ref[...] = 0.5 * folded

    stages = (adjoint, send_one, send_two, send_three, send_pair, mix, send_g2, send_g3, forward)
    lag = (0, 0, 1, 2, 3, 4, 5, 6, 7)
    for t in range(chunks + lag[-1]):
        if t == 4:
            take_stats()
        j = t - lag[-1]
        if t < chunks:
            adjoint(t)
        if t == 0:
            pl.semaphore_wait(barrier, n)

            def start_stats(p, carry):
                stat_copy(p, me).start()
                return carry

            lax.fori_loop(1, n, start_stats, 0)
            vert_copy(lev).start()
        if t == 3:
            vert_copy(other).wait_recv()
        for stage, late in reversed(tuple(zip(stages[1:-1], lag[1:-1]))):
            if 0 <= t - late < chunks:
                stage(t - late)
        if t - lag[5] == chunks - 1:
            send_parts()
        if 0 <= j < chunks:
            forward(j)
    take_parts()

    for j in range(chunks):
        for copy in one(j) + two(j) + three(j, y, x) + four(j, y, x) + (pair_copy(j, lev),):
            copy.wait_send()

        def finish_outer(p, carry):
            outer_copy(j, p).wait_send()
            lifted_copy(j, p, h).wait_send()
            return carry

        lax.fori_loop(1, outer, finish_outer, 0)

    def finish(p, carry):
        stat_copy(p, me).wait_send()
        part_copy(p, me).wait_send()
        return carry

    lax.fori_loop(1, n, finish, 0)
    vert_copy(lev).wait_send()


def per_device(perturbations, gradient, horizontal, area, vertical):
    members, levels, columns = perturbations.shape
    vectors = gradient.shape[0]
    modes = horizontal.shape[0]
    n = lax.axis_size("col")
    sizes = (members, levels, vectors, modes, columns)
    chunks = modes * vectors // LANES
    tiles = max(2, -(-members // n))
    rows = tiles * levels
    outer = n // 4
    most = (tiles + 1) // 2 * levels
    f32 = jnp.float32
    vmem = pl.BlockSpec(memory_space=pltpu.VMEM)
    dma = pltpu.SemaphoreType.DMA

    increment, background = pl.pallas_call(
        functools.partial(kernel, sizes, n),
        out_shape=(
            jax.ShapeDtypeStruct((vectors, levels, columns), f32),
            jax.ShapeDtypeStruct((8, LANES), f32),
        ),
        in_specs=[vmem] * 5,
        out_specs=(vmem, vmem),
        scratch_shapes=[
            pltpu.VMEM((levels, 2 * members, columns), jnp.bfloat16),
            pltpu.VMEM((levels, vectors, columns), f32),
            pltpu.VMEM((levels, vectors, columns), f32),
            pltpu.VMEM((chunks, outer, 2, 2, rows, LANES), f32),
            pltpu.VMEM((chunks, outer, 2, most, LANES), f32),
            pltpu.VMEM((chunks, outer, 2, most, LANES), f32),
            pltpu.VMEM((chunks, outer, rows, LANES), f32),
            pltpu.VMEM((chunks, outer, rows, LANES), f32),
            pltpu.VMEM((chunks, 2, rows, LANES), f32),
            pltpu.VMEM((chunks, outer, 2, 2, rows, LANES), f32),
            pltpu.VMEM((8, LANES), f32),
            pltpu.VMEM((n, 8, LANES), f32),
            pltpu.VMEM((2, levels, LANES), f32),
            pltpu.VMEM((8, LANES), f32),
            pltpu.VMEM((n, 8, LANES), f32),
            pltpu.VMEM((8, LANES), f32),
            pltpu.VMEM((modes, columns), f32),
            dma((chunks, 8)), dma((chunks, 8)),
            dma((chunks, outer)), dma((chunks, outer)),
            dma((chunks, outer)), dma((chunks, outer)),
            dma((chunks,)), dma((chunks,)),
            dma((n,)), dma((n,)), dma((n,)), dma((n,)),
            dma((1,)), dma((1,)),
        ],
        compiler_params=pltpu.CompilerParams(collective_id=0, has_side_effects=True),
        name="covariance",
    )(perturbations, gradient, horizontal, area.reshape(1, columns), vertical.T)
    return increment, background[0, :vectors]


def solution(mesh):
    return jax.shard_map(
        per_device,
        mesh=mesh,
        in_specs=(
            P(None, "lev", "col"),
            P(None, "lev", "col"),
            P(None, "col"),
            P("col"),
            P(None, "lev"),
        ),
        out_specs=(P(None, "lev", "col"), P()),
        check_vma=False,
    )
```

```python
import functools

import jax
import jax.numpy as jnp
from jax import lax
from jax.experimental import pallas as pl
from jax.experimental.pallas import tpu as pltpu
from jax.sharding import PartitionSpec as P

LANES = 128
NT = (((1,), (1,)), ((), ()))
TN = (((0,), (0,)), ((), ()))
NN = (((1,), (0,)), ((), ()))
UNROLL = 2


def split(x):
    high = x.astype(jnp.bfloat16)
    low = (x - high.astype(jnp.float32)).astype(jnp.bfloat16)
    return high, low


def exact_dot(a, b, dims):
    return lax.dot_general(
        a, b, dims, precision=lax.Precision.HIGHEST, preferred_element_type=jnp.float32
    )


def kernel(
    sizes, n, pert_ref, grad_ref, hor_ref, area_ref, vert_ref, out_ref, bg_ref,
    halves, weighted, acc, terms, first_a, first_b, second, third, reduced, lifted,
    stat_ref, stats, verticals, sums, parts, weights, scaled,
    send_h, recv_h, send_g, recv_g, send_l, recv_l, send_p, recv_p,
    send_s, recv_s, send_b, recv_b, send_v, recv_v,
):
    members, levels, vectors, modes, columns = sizes
    group = LANES // vectors
    chunks = modes // group
    vmodes = vert_ref.shape[1]
    rows = terms.shape[4]
    tiles = rows // levels
    outer = n // 4
    used = members * levels
    me = lax.axis_index("col")
    lev = lax.axis_index("lev")
    other = 1 - lev
    x = lax.rem(me, 2)
    y = lax.rem(lax.div(me, 2), 2)
    h = lax.div(me, 4)
    not_x, not_y = 1 - x, 1 - y
    x_peer = (4 * h + 2 * y + not_x, lev)
    y_peer = (4 * h + 2 * not_y + x, lev)
    mesh_id = pl.DeviceIdType.MESH
    barrier = pltpu.get_barrier_semaphore()

    def greet(p, carry):
        pl.semaphore_signal(
            barrier, inc=1, device_id=(lax.rem(me + p, n), lev), device_id_type=mesh_id
        )
        return carry

    lax.fori_loop(1, n, greet, 0)
    pl.semaphore_signal(barrier, inc=1, device_id=(me, other), device_id_type=mesh_id)

    def remote(src, dst, send, recv, device):
        return pltpu.make_async_remote_copy(
            src_ref=src, dst_ref=dst, send_sem=send, recv_sem=recv,
            device_id=device, device_id_type=mesh_id,
        )

    def halfway(j):
        count = (tiles + 1 - j % 2) // 2 * levels
        return pl.ds(0, count), pl.ds(count, rows - count), count, rows - count

    def half_copy(j, i, src, dst, device):
        return remote(src, dst, send_h.at[j, i], recv_h.at[j, i], device)

    def one(j):
        a, b, na, nb = halfway(j)
        return (
            half_copy(j, 0, terms.at[j, :, :, not_x, a], first_a.at[j, :, :, pl.ds(0, na)], x_peer),
            half_copy(j, 1, terms.at[j, :, not_y, :, b], first_b.at[j, :, :, pl.ds(0, nb)], y_peer),
        )

    def two(j):
        a, b, na, nb = halfway(j)
        return (
            half_copy(j, 2, first_a.at[j, :, not_y, pl.ds(0, na)], second.at[j, :, a], y_peer),
            half_copy(j, 3, first_b.at[j, :, not_x, pl.ds(0, nb)], second.at[j, :, b], x_peer),
        )

    def outer_copy(j, p):
        there = lax.rem(h + p, outer)
        device = (4 * there + 2 * y + x, lev)
        return remote(
            second.at[j, there], third.at[j, p], send_g.at[j, p], recv_g.at[j, p], device
        )

    def pair_copy(j, slot):
        block = reduced.at[j, slot]
        return remote(block, block, send_p.at[j], recv_p.at[j], (me, other))

    def lifted_copy(j, p, slot):
        there = lax.rem(h + p, outer)
        device = (4 * there + 2 * y + x, lev)
        block = lifted.at[j, slot, y, x]
        return remote(block, block, send_l.at[j, p], recv_l.at[j, p], device)

    def three(j, yy, xx):
        a, b, _, _ = halfway(j)
        block_a = lifted.at[j, :, yy, x, a]
        block_b = lifted.at[j, :, y, xx, b]
        return (
            half_copy(j, 4, block_a, block_a, y_peer),
            half_copy(j, 5, block_b, block_b, x_peer),
        )

    def four(j, yy, xx):
        a, b, _, _ = halfway(j)
        block_a = lifted.at[j, :, :, xx, a]
        block_b = lifted.at[j, :, yy, :, b]
        return (
            half_copy(j, 6, block_a, block_a, x_peer),
            half_copy(j, 7, block_b, block_b, y_peer),
        )

    def stat_copy(p, slot):
        peer = lax.rem(me + p, n)
        return remote(stat_ref, stats.at[slot], send_s.at[p], recv_s.at[p], (peer, lev))

    def part_copy(p, slot):
        peer = lax.rem(me + p, n)
        block = parts.at[slot]
        return remote(block, block, send_b.at[p], recv_b.at[p], (peer, lev))

    def vert_copy(slot):
        block = verticals.at[slot]
        return remote(block, block, send_v.at[0], recv_v.at[0], (me, other))

    area = area_ref[...]
    power = jnp.sum(area * hor_ref[...] * hor_ref[...], axis=1, keepdims=True)
    lane = lax.broadcasted_iota(jnp.int32, (modes, LANES), 1)
    row = lax.broadcasted_iota(jnp.int32, (modes, LANES), 0)
    powers = jnp.sum(
        jnp.where(lane == row, jnp.broadcast_to(power, (modes, LANES)), 0.0),
        axis=0, keepdims=True,
    )
    total = jnp.broadcast_to(jnp.sum(area, axis=1, keepdims=True), (1, LANES))
    stat_row = jnp.where(lane[:1] == modes, total, powers)
    stat_ref[...] = jnp.broadcast_to(stat_row, stat_ref.shape)
    verticals[lev] = jnp.zeros(verticals.shape[1:], jnp.float32)
    verticals[lev, :, :vmodes] = vert_ref[...]
    if used < n * rows:
        for j in range(chunks):
            flat = terms.at[j].reshape(n * rows, LANES)
            flat[used:, :] = jnp.zeros((n * rows - used, LANES), jnp.float32)
    for c in range(0, columns, LANES):
        lanes = slice(c, c + LANES)
        for k in range(0, members, 16):
            high, low = split(jnp.swapaxes(pert_ref[k : k + 16, :, lanes], 0, 1))
            halves[:, k : k + 16, lanes] = high
            halves[:, members + k : members + k + 16, lanes] = low
        for v in range(0, vectors, 8):
            block = jnp.swapaxes(grad_ref[v : v + 8, :, lanes], 0, 1)
            weighted[:, v : v + 8, lanes] = block * area[:, lanes]

    def over_levels(step):
        def body(i, carry):
            for u in range(UNROLL):
                step(i * UNROLL + u)
            return carry

        lax.fori_loop(0, levels // UNROLL, body, 0)

    def adjoint(j):
        flat = terms.at[j].reshape(n * rows, LANES)

        def step(l):
            base = weighted[l]
            products = jnp.concatenate(
                [base * hor_ref[b : b + 1, :] for b in range(j * group, (j + 1) * group)],
                axis=0,
            )
            both = jnp.concatenate(split(products), axis=0)
            out = lax.dot_general(halves[l], both, NT, preferred_element_type=jnp.float32)
            flat[pl.ds(l, members, stride=levels), :] = out[:members, :LANES] + (
                out[members:, :LANES] + out[:members, LANES:]
            )

        over_levels(step)

    def start(copies):
        for copy in copies:
            copy.start()

    def send_one(j):
        start(one(j))

    def send_two(j):
        a, b, na, nb = halfway(j)
        one_a, one_b = one(j)
        two_a, two_b = two(j)
        one_a.wait_recv()

        def add_a(i, carry):
            first_a[j, i, not_y, :na] += terms[j, i, not_y, x, a]
            return carry

        lax.fori_loop(0, outer, add_a, 0)
        two_a.start()
        one_b.wait_recv()

        def add_b(i, carry):
            first_b[j, i, not_x, :nb] += terms[j, i, y, not_x, b]
            return carry

        lax.fori_loop(0, outer, add_b, 0)
        two_b.start()

    def add_second(j, there):
        a, b, na, nb = halfway(j)
        second[j, there, a] += terms[j, there, y, x, a] + first_a[j, there, y, :na]
        second[j, there, b] += terms[j, there, y, x, b] + first_b[j, there, x, :nb]

    def send_three(j):
        for copy in two(j):
            copy.wait_recv()

        def send_outer(p, carry):
            add_second(j, lax.rem(h + p, outer))
            outer_copy(j, p).start()
            return carry

        lax.fori_loop(1, outer, send_outer, 0)
        add_second(j, h)
        reduced[j, lev] = second[j, h]

    def send_pair(j):
        def take(p, carry):
            outer_copy(j, p).wait_recv()
            reduced[j, lev] += third[j, p]
            return carry

        lax.fori_loop(1, outer, take, 0)
        pair_copy(j, lev).start()

    def mix(j):
        pair_copy(j, other).wait_recv()

        def wide(index):
            block = reduced[j, index]
            return jnp.concatenate(
                [block[i * levels : (i + 1) * levels] for i in range(tiles)], axis=1
            )

        control = exact_dot(verticals[0][:, :vmodes], wide(0), TN) + exact_dot(
            verticals[1][:, :vmodes], wide(1), TN
        )
        raised = exact_dot(vert_ref[...], control, NN)
        square = jnp.zeros((1, LANES), jnp.float32)
        for i in range(tiles):
            lanes = slice(i * LANES, (i + 1) * LANES)
            lifted[j, h, y, x, i * levels : (i + 1) * levels, :] = raised[:, lanes]
            square = square + jnp.sum(
                control[:, lanes] * control[:, lanes], axis=0, keepdims=True
            )
        sums[j : j + 1, :] = square

        def start_lifted(p, carry):
            lifted_copy(j, p, h).start()
            return carry

        lax.fori_loop(1, outer, start_lifted, 0)

    def send_g2(j):
        def take_lifted(p, carry):
            lifted_copy(j, p, lax.rem(h + outer - p, outer)).wait_recv()
            return carry

        lax.fori_loop(1, outer, take_lifted, 0)
        start(three(j, y, x))

    def send_g3(j):
        three_a, three_b = three(j, not_y, not_x)
        four_a, four_b = four(j, y, x)
        three_a.wait_recv()
        four_a.start()
        three_b.wait_recv()
        four_b.start()

    def forward(j):
        for copy in four(j, not_y, not_x):
            copy.wait_recv()
        flat = lifted.at[j].reshape(n * rows, LANES)
        width = 256

        def step(l):
            high, low = split(flat[pl.ds(l, members, stride=levels), :])
            lhs = jnp.concatenate([high, high, low], axis=0)
            for c in range(0, columns, width):
                cols = slice(c, c + width)
                rhs = jnp.concatenate([halves[l, :, cols], halves[l, :members, cols]], axis=0)
                spread = lax.dot_general(lhs, rhs, TN, preferred_element_type=jnp.float32)
                value = None if j == 0 else acc[l, :, cols]
                for g in range(group):
                    b = j * group + g
                    term = spread[g * vectors : (g + 1) * vectors] * scaled[b : b + 1, cols]
                    value = term if value is None else value + term
                acc[l, :, cols] = value

        over_levels(step)

    def finish_out():
        for c in range(0, columns, LANES):
            lanes = slice(c, c + LANES)
            for v in range(0, vectors, 8):
                out_ref[v : v + 8, :, lanes] = jnp.swapaxes(acc[:, v : v + 8, lanes], 0, 1)

    def take_stats():
        stats[me] = stat_ref[...]

        def take(p, carry):
            stat_copy(p, lax.rem(me + n - p, n)).wait_recv()
            return carry

        lax.fori_loop(1, n, take, 0)
        stat = lax.fori_loop(
            0, n, lambda i, c: c + stats[i], jnp.zeros(stat_ref.shape, jnp.float32)
        )
        spread = jnp.broadcast_to(stat[:1], (modes, LANES))
        power = jnp.sum(jnp.where(lane == row, spread, 0.0), axis=1, keepdims=True)
        whole = jnp.sum(jnp.where(lane == modes, spread, 0.0), axis=1, keepdims=True)
        factor = 1.0 / jnp.sqrt(modes * (power / whole + 1e-06))
        scale = factor * (columns * n / whole)
        scaled[...] = hor_ref[...] * (factor * scale)
        placed = jnp.where(
            lax.div(lane, vectors) == lax.rem(row, group),
            jnp.broadcast_to(scale, lane.shape), 0.0,
        )
        for j in range(chunks):
            weights[j : j + 1, :] = jnp.sum(
                placed[j * group : (j + 1) * group], axis=0, keepdims=True
            )

    def send_parts():
        part = jnp.zeros((1, LANES), jnp.float32)
        for j in range(chunks):
            weight = weights[j : j + 1, :]
            part = part + sums[j : j + 1, :] * weight * weight
        parts[me] = jnp.broadcast_to(part, parts.shape[1:])

        def start_parts(p, carry):
            part_copy(p, me).start()
            return carry

        lax.fori_loop(1, n, start_parts, 0)

    def take_parts():
        def take(p, carry):
            part_copy(p, lax.rem(me + n - p, n)).wait_recv()
            return carry

        lax.fori_loop(1, n, take, 0)
        part = lax.fori_loop(
            0, n, lambda i, c: c + parts[i], jnp.zeros(parts.shape[1:], jnp.float32)
        )
        folded = part
        for g in range(1, group):
            folded = folded + pltpu.roll(part, g * vectors, 1)
        bg_ref[...] = 0.5 * folded

    stages = (adjoint, send_one, send_two, send_three, send_pair, mix, send_g2, send_g3, forward)
    lag = (0, 0, 1, 2, 3, 4, 5, 6, 7)
    for t in range(chunks + lag[-1]):
        if t == 4:
            take_stats()
        j = t - lag[-1]
        if t < chunks:
            adjoint(t)
        if t == 0:
            pl.semaphore_wait(barrier, n)

            def start_stats(p, carry):
                stat_copy(p, me).start()
                return carry

            lax.fori_loop(1, n, start_stats, 0)
            vert_copy(lev).start()
        if t == 3:
            vert_copy(other).wait_recv()
        for stage, late in reversed(tuple(zip(stages[1:-1], lag[1:-1]))):
            if 0 <= t - late < chunks:
                stage(t - late)
        if t - lag[5] == chunks - 1:
            send_parts()
        if 0 <= j < chunks:
            forward(j)
    finish_out()
    take_parts()

    for j in range(chunks):
        for copy in one(j) + two(j) + three(j, y, x) + four(j, y, x) + (pair_copy(j, lev),):
            copy.wait_send()

        def finish_outer(p, carry):
            outer_copy(j, p).wait_send()
            lifted_copy(j, p, h).wait_send()
            return carry

        lax.fori_loop(1, outer, finish_outer, 0)

    def finish(p, carry):
        stat_copy(p, me).wait_send()
        part_copy(p, me).wait_send()
        return carry

    lax.fori_loop(1, n, finish, 0)
    vert_copy(lev).wait_send()


def per_device(perturbations, gradient, horizontal, area, vertical):
    members, levels, columns = perturbations.shape
    vectors = gradient.shape[0]
    modes = horizontal.shape[0]
    n = lax.axis_size("col")
    sizes = (members, levels, vectors, modes, columns)
    chunks = modes * vectors // LANES
    tiles = max(2, -(-members // n))
    rows = tiles * levels
    outer = n // 4
    most = (tiles + 1) // 2 * levels
    f32 = jnp.float32
    vmem = pl.BlockSpec(memory_space=pltpu.VMEM)
    dma = pltpu.SemaphoreType.DMA

    held = chunks * n * rows * LANES * 4 * 9 // 2
    limit = min(60 * 2**20, held + 14 * 2**20)
    increment, background = pl.pallas_call(
        functools.partial(kernel, sizes, n),
        out_shape=(
            jax.ShapeDtypeStruct((vectors, levels, columns), f32),
            jax.ShapeDtypeStruct((8, LANES), f32),
        ),
        in_specs=[vmem] * 5,
        out_specs=(vmem, vmem),
        scratch_shapes=[
            pltpu.VMEM((levels, 2 * members, columns), jnp.bfloat16),
            pltpu.VMEM((levels, vectors, columns), f32),
            pltpu.VMEM((levels, vectors, columns), f32),
            pltpu.VMEM((chunks, outer, 2, 2, rows, LANES), f32),
            pltpu.VMEM((chunks, outer, 2, most, LANES), f32),
            pltpu.VMEM((chunks, outer, 2, most, LANES), f32),
            pltpu.VMEM((chunks, outer, rows, LANES), f32),
            pltpu.VMEM((chunks, outer, rows, LANES), f32),
            pltpu.VMEM((chunks, 2, rows, LANES), f32),
            pltpu.VMEM((chunks, outer, 2, 2, rows, LANES), f32),
            pltpu.VMEM((8, LANES), f32),
            pltpu.VMEM((n, 8, LANES), f32),
            pltpu.VMEM((2, levels, LANES), f32),
            pltpu.VMEM((8, LANES), f32),
            pltpu.VMEM((n, 8, LANES), f32),
            pltpu.VMEM((8, LANES), f32),
            pltpu.VMEM((modes, columns), f32),
            dma((chunks, 8)), dma((chunks, 8)),
            dma((chunks, outer)), dma((chunks, outer)),
            dma((chunks, outer)), dma((chunks, outer)),
            dma((chunks,)), dma((chunks,)),
            dma((n,)), dma((n,)), dma((n,)), dma((n,)),
            dma((1,)), dma((1,)),
        ],
        compiler_params=pltpu.CompilerParams(
            collective_id=0, has_side_effects=True, vmem_limit_bytes=limit
        ),
        name="covariance",
    )(perturbations, gradient, horizontal, area.reshape(1, columns), vertical.T)
    return increment, background[0, :vectors]


def solution(mesh):
    return jax.shard_map(
        per_device,
        mesh=mesh,
        in_specs=(
            P(None, "lev", "col"),
            P(None, "lev", "col"),
            P(None, "col"),
            P("col"),
            P(None, "lev"),
        ),
        out_specs=(P(None, "lev", "col"), P()),
        check_vma=False,
    )
```

```python
import functools

import jax
import jax.numpy as jnp
from jax import lax
from jax.experimental import pallas as pl
from jax.experimental.pallas import tpu as pltpu
from jax.sharding import PartitionSpec as P

LANES = 128
NT = (((1,), (1,)), ((), ()))
TN = (((0,), (0,)), ((), ()))
NN = (((1,), (0,)), ((), ()))
UNROLL = 2
BLOCKS = 4


def split(x):
    high = x.astype(jnp.bfloat16)
    low = (x - high.astype(jnp.float32)).astype(jnp.bfloat16)
    return high, low


def exact_dot(a, b, dims):
    return lax.dot_general(
        a, b, dims, precision=lax.Precision.HIGHEST, preferred_element_type=jnp.float32
    )


def timetable(*stages):
    starts = (3.5, 8.3, 12.8, 17.0, 22.9, 29.1, 32.5, 40.7)
    paces = (2.05, 2.4, 2.7, 2.6, 2.9, 2.9, 3.0, 2.3)
    return zip(stages, starts, paces)


def kernel(
    sizes, n, pert_hbm, grad_hbm, hor_hbm, area_hbm, vert_hbm, out_ref, bg_ref,
    pert_ref, grad_ref, hor_ref, area_ref, vert_ref,
    halves, weighted, acc, terms, first_a, first_b, second, third, raised, lifted,
    totals, verticals, sums, weights, scaled,
    load_p, load_s, send_h, recv_h, send_g, recv_g, send_l, recv_l, send_m, recv_m,
    send_t, recv_t, send_v, recv_v,
):
    members, levels, vectors, modes, columns = sizes
    group = LANES // vectors
    chunks = modes // group
    vmodes = vert_ref.shape[1]
    rows = terms.shape[4]
    tiles = rows // levels
    outer = n // 4
    used = members * levels
    me = lax.axis_index("col")
    lev = lax.axis_index("lev")
    other = 1 - lev
    x = lax.rem(me, 2)
    y = lax.rem(lax.div(me, 2), 2)
    h = lax.div(me, 4)
    not_x, not_y = 1 - x, 1 - y
    x_peer = (4 * h + 2 * y + not_x, lev)
    y_peer = (4 * h + 2 * not_y + x, lev)
    partner = (me, other)
    mesh_id = pl.DeviceIdType.MESH
    barrier = pltpu.get_barrier_semaphore()

    def along(p):
        return 4 * lax.rem(h + p, outer) + 2 * y + x

    def greet(device):
        pl.semaphore_signal(barrier, inc=1, device_id=device, device_id_type=mesh_id)

    def greet_outer(p, carry):
        greet((along(p), lev))
        greet((along(p), other))
        return carry

    for device in (x_peer, y_peer, partner):
        greet(device)
    lax.fori_loop(1, outer, greet_outer, 0)

    wide_block = columns // BLOCKS

    def load_block(q):
        part = pl.ds(q * wide_block, wide_block)
        return (
            pltpu.make_async_copy(
                pert_hbm.at[:, :, part], pert_ref.at[:, :, part], load_p.at[0, q]
            ),
            pltpu.make_async_copy(
                grad_hbm.at[:, :, part], grad_ref.at[:, :, part], load_p.at[1, q]
            ),
        )

    small = [
        pltpu.make_async_copy(source, target, load_s.at[i])
        for i, (source, target) in enumerate(
            ((area_hbm, area_ref), (hor_hbm, hor_ref), (vert_hbm, vert_ref))
        )
    ]
    for copy in small:
        copy.start()
    for q in range(BLOCKS):
        for copy in load_block(q):
            copy.start()

    def remote(src, dst, send, recv, device):
        return pltpu.make_async_remote_copy(
            src_ref=src, dst_ref=dst, send_sem=send, recv_sem=recv,
            device_id=device, device_id_type=mesh_id,
        )

    def halfway(j):
        count = (tiles + 1 - j % 2) // 2 * levels
        return pl.ds(0, count), pl.ds(count, rows - count), count, rows - count

    def half_copy(j, i, src, dst, device):
        return remote(src, dst, send_h.at[j, i], recv_h.at[j, i], device)

    def one(j):
        a, b, na, nb = halfway(j)
        return (
            half_copy(j, 0, terms.at[j, :, :, not_x, a], first_a.at[j, :, :, pl.ds(0, na)], x_peer),
            half_copy(j, 1, terms.at[j, :, not_y, :, b], first_b.at[j, :, :, pl.ds(0, nb)], y_peer),
        )

    def two(j):
        a, b, na, nb = halfway(j)
        return (
            half_copy(j, 2, first_a.at[j, :, not_y, pl.ds(0, na)], second.at[j, :, a], y_peer),
            half_copy(j, 3, first_b.at[j, :, not_x, pl.ds(0, nb)], second.at[j, :, b], x_peer),
        )

    def keeper(j):
        return j % 2

    def outer_copy(j, p, source):
        return remote(
            second.at[j, lax.rem(h + p, outer)], third.at[j, source, p],
            send_g.at[j, p], recv_g.at[j, source, p], (along(p), keeper(j)),
        )

    def lifted_copy(j, p, slot):
        block = lifted.at[j, slot, y, x]
        return remote(block, block, send_l.at[j, p], recv_l.at[j, p], (along(p), lev))

    def raised_copy(j, p, slot):
        return remote(
            raised.at[j], lifted.at[j, slot, y, x],
            send_m.at[j, p], recv_m.at[j, p], (along(p), other),
        )

    def three(j, yy, xx):
        a, b, _, _ = halfway(j)
        block_a = lifted.at[j, :, yy, x, a]
        block_b = lifted.at[j, :, y, xx, b]
        return (
            half_copy(j, 4, block_a, block_a, y_peer),
            half_copy(j, 5, block_b, block_b, x_peer),
        )

    def four(j, yy, xx):
        a, b, _, _ = halfway(j)
        block_a = lifted.at[j, :, :, xx, a]
        block_b = lifted.at[j, :, yy, :, b]
        return (
            half_copy(j, 6, block_a, block_a, x_peer),
            half_copy(j, 7, block_b, block_b, y_peer),
        )

    def vert_copy(slot):
        block = verticals.at[slot]
        return remote(block, block, send_v.at[0], recv_v.at[0], partner)

    def total_copy(k, source, target, device):
        return remote(
            totals.at[k, source], totals.at[k, target],
            send_t.at[k, target], recv_t.at[k, target], device,
        )

    def total_outer(k, p):
        return total_copy(k, 6, 6 + p, (along(p), lev))

    def total_x(k):
        return total_copy(k, 0, 1, x_peer)

    def total_y(k):
        return total_copy(k, 2, 3, y_peer)

    def total_c(k):
        return total_copy(k, 4, 5, partner)

    def send_total_x(k):
        total_x(k).start()

    def send_total_y(k):
        total_x(k).wait_recv()
        totals[k, 2] = totals[k, 0] + totals[k, 1]
        total_y(k).start()

    def send_total_c(k):
        total_y(k).wait_recv()
        totals[k, 4] = totals[k, 2] + totals[k, 3]
        total_c(k).start()

    def send_total_outer(k):
        total_c(k).wait_recv()
        totals[k, 6] = totals[k, 4] + totals[k, 5]

        def send(p, carry):
            total_outer(k, p).start()
            return carry

        lax.fori_loop(1, outer, send, 0)

    def take_total(k):
        def take(p, carry):
            total_outer(k, p).wait_recv()
            return carry + totals[k, 6 + p]

        return lax.fori_loop(1, outer, take, totals[k, 6])

    lane = lax.broadcasted_iota(jnp.int32, (modes, LANES), 1)
    row = lax.broadcasted_iota(jnp.int32, (modes, LANES), 0)
    sums[...] = jnp.zeros(sums.shape, jnp.float32)
    verticals[lev] = jnp.zeros(verticals.shape[1:], jnp.float32)
    if used < n * rows:
        for j in range(chunks):
            flat = terms.at[j].reshape(n * rows, LANES)
            flat[used:, :] = jnp.zeros((n * rows - used, LANES), jnp.float32)
    for copy in small:
        copy.wait()
    area = area_ref[...]
    verticals[lev, :, :vmodes] = vert_ref[...]

    def prepare():
        for q in range(BLOCKS):
            for copy in load_block(q):
                copy.wait()
            for c in range(q * wide_block, (q + 1) * wide_block, LANES):
                lanes = slice(c, c + LANES)
                for k in range(0, members, 16):
                    high, low = split(jnp.swapaxes(pert_ref[k : k + 16, :, lanes], 0, 1))
                    halves[:, k : k + 16, lanes] = high
                    halves[:, members + k : members + k + 16, lanes] = low
                for v in range(0, vectors, 8):
                    block = jnp.swapaxes(grad_ref[v : v + 8, :, lanes], 0, 1)
                    weighted[:, v : v + 8, lanes] = block * area[:, lanes]

    def statistics():
        power = jnp.sum(area * hor_ref[...] * hor_ref[...], axis=1, keepdims=True)
        powers = jnp.sum(
            jnp.where(lane == row, jnp.broadcast_to(power, (modes, LANES)), 0.0),
            axis=0, keepdims=True,
        )
        total = jnp.broadcast_to(jnp.sum(area, axis=1, keepdims=True), (1, LANES))
        stat_row = jnp.where(lane[:1] == modes, total, powers)
        totals[0, 0] = jnp.broadcast_to(stat_row, totals.shape[2:])

    def over_levels(step):
        def body(i, carry):
            for u in range(UNROLL):
                step(i * UNROLL + u)
            return carry

        lax.fori_loop(0, levels // UNROLL, body, 0)

    def adjoint(j):
        flat = terms.at[j].reshape(n * rows, LANES)

        def step(l):
            base = weighted[l]
            products = jnp.concatenate(
                [base * hor_ref[b : b + 1, :] for b in range(j * group, (j + 1) * group)],
                axis=0,
            )
            both = jnp.concatenate(split(products), axis=0)
            out = lax.dot_general(halves[l], both, NT, preferred_element_type=jnp.float32)
            flat[pl.ds(l, members, stride=levels), :] = out[:members, :LANES] + (
                out[members:, :LANES] + out[:members, LANES:]
            )

        over_levels(step)

    def send_one(j):
        for copy in one(j):
            copy.start()

    def send_two(j):
        a, b, na, nb = halfway(j)
        one_a, one_b = one(j)
        two_a, two_b = two(j)

        def add_a(i, carry):
            first_a[j, i, not_y, :na] += terms[j, i, not_y, x, a]
            return carry

        def add_b(i, carry):
            first_b[j, i, not_x, :nb] += terms[j, i, y, not_x, b]
            return carry

        one_a.wait_recv()
        lax.fori_loop(0, outer, add_a, 0)
        two_a.start()
        one_b.wait_recv()
        lax.fori_loop(0, outer, add_b, 0)
        two_b.start()

    def add_second(j, there):
        a, b, na, nb = halfway(j)
        second[j, there, a] += terms[j, there, y, x, a] + first_a[j, there, y, :na]
        second[j, there, b] += terms[j, there, y, x, b] + first_b[j, there, x, :nb]

    def send_three(j):
        for copy in two(j):
            copy.wait_recv()

        def send_outer(p, carry):
            add_second(j, lax.rem(h + p, outer))
            outer_copy(j, p, lev).start()
            return carry

        lax.fori_loop(1, outer, send_outer, 0)
        add_second(j, h)

        @pl.when(lev != keeper(j))
        def _():
            outer_copy(j, 0, lev).start()

    def mix(j):
        @pl.when(lev == keeper(j))
        def _():
            def take(p, carry):
                outer_copy(j, p, lev).wait_recv()
                second[j, h] += third[j, lev, p]
                outer_copy(j, p, other).wait_recv()
                third[j, other, 0] += third[j, other, p]
                return carry

            outer_copy(j, 0, other).wait_recv()
            lax.fori_loop(1, outer, take, 0)

            def wide(block):
                return jnp.concatenate(
                    [block[i * levels : (i + 1) * levels] for i in range(tiles)], axis=1
                )

            far = verticals[other][:, :vmodes]
            control = exact_dot(vert_ref[...], wide(second[j, h]), TN) + exact_dot(
                far, wide(third[j, other, 0]), TN
            )
            near_lifted = exact_dot(vert_ref[...], control, NN)
            far_lifted = exact_dot(far, control, NN)
            square = jnp.zeros((1, LANES), jnp.float32)
            for i in range(tiles):
                lanes = slice(i * LANES, (i + 1) * LANES)
                part = slice(i * levels, (i + 1) * levels)
                lifted[j, h, y, x, part, :] = near_lifted[:, lanes]
                raised[j, part, :] = far_lifted[:, lanes]
                square = square + jnp.sum(
                    control[:, lanes] * control[:, lanes], axis=0, keepdims=True
                )
            sums[j : j + 1, :] = square

            def start_lifted(p, carry):
                lifted_copy(j, p, h).start()
                raised_copy(j, p, h).start()
                return carry

            raised_copy(j, 0, h).start()
            lax.fori_loop(1, outer, start_lifted, 0)

    def send_g2(j):
        @pl.when(lev == keeper(j))
        def _():
            def take(p, carry):
                lifted_copy(j, p, lax.rem(h + outer - p, outer)).wait_recv()
                return carry

            lax.fori_loop(1, outer, take, 0)

        @pl.when(lev != keeper(j))
        def _():
            def take(p, carry):
                raised_copy(j, p, lax.rem(h + outer - p, outer)).wait_recv()
                return carry

            lax.fori_loop(0, outer, take, 0)

        for copy in three(j, y, x):
            copy.start()

    def send_g3(j):
        three_a, three_b = three(j, not_y, not_x)
        four_a, four_b = four(j, y, x)
        three_a.wait_recv()
        four_a.start()
        three_b.wait_recv()
        four_b.start()

    def forward(j):
        for copy in four(j, not_y, not_x):
            copy.wait_recv()
        flat = lifted.at[j].reshape(n * rows, LANES)
        width = 256

        def step(l):
            high, low = split(flat[pl.ds(l, members, stride=levels), :])
            lhs = jnp.concatenate([high, high, low], axis=0)
            for c in range(0, columns, width):
                cols = slice(c, c + width)
                rhs = jnp.concatenate([halves[l, :, cols], halves[l, :members, cols]], axis=0)
                spread = lax.dot_general(lhs, rhs, TN, preferred_element_type=jnp.float32)
                value = None if j == 0 else acc[l, :, cols]
                for g in range(group):
                    b = j * group + g
                    term = spread[g * vectors : (g + 1) * vectors] * scaled[b : b + 1, cols]
                    value = term if value is None else value + term
                acc[l, :, cols] = value

        over_levels(step)

    def take_stats(k):
        stat = 0.5 * take_total(k)
        spread = jnp.broadcast_to(stat[:1], (modes, LANES))
        power = jnp.sum(jnp.where(lane == row, spread, 0.0), axis=1, keepdims=True)
        whole = jnp.sum(jnp.where(lane == modes, spread, 0.0), axis=1, keepdims=True)
        factor = 1.0 / jnp.sqrt(modes * (power / whole + 1e-06))
        scale = factor * (columns * n / whole)
        scaled[...] = hor_ref[...] * (factor * scale)
        placed = jnp.where(
            lax.div(lane, vectors) == lax.rem(row, group),
            jnp.broadcast_to(scale, lane.shape), 0.0,
        )
        for j in range(chunks):
            weights[j : j + 1, :] = jnp.sum(
                placed[j * group : (j + 1) * group], axis=0, keepdims=True
            )

    def gather_sums(k):
        part = jnp.zeros((1, LANES), jnp.float32)
        for j in range(chunks):
            weight = weights[j : j + 1, :]
            part = part + sums[j : j + 1, :] * weight * weight
        totals[k, 0] = jnp.broadcast_to(part, totals.shape[2:])
        send_total_x(k)

    def finish_sums(k):
        part = take_total(k)
        folded = part
        for g in range(1, group):
            folded = folded + pltpu.roll(part, g * vectors, 1)
        bg_ref[...] = 0.5 * folded

    def meet(k):
        pl.semaphore_wait(barrier, 3 + 2 * (outer - 1))
        vert_copy(lev).start()

    def take_vert(k):
        vert_copy(other).wait_recv()

    def set_stats(k):
        statistics()
        send_total_x(k)

    def finish_out(k):
        for c in range(0, columns, LANES):
            lanes = slice(c, c + LANES)
            for v in range(0, vectors, 8):
                out_ref[v : v + 8, :, lanes] = jnp.swapaxes(acc[:, v : v + 8, lanes], 0, 1)

    plan = [
        (start + pace * j, stage, j)
        for stage, start, pace in timetable(
            adjoint, send_one, send_two, send_three, mix, send_g2, send_g3, forward
        )
        for j in range(chunks)
    ]
    last = chunks - 5
    plan += [
        (8.2, meet, 0), (8.65, set_stats, 0), (13.0, send_total_y, 0), (16.7, send_total_c, 0),
        (19.0, send_total_outer, 0), (20.0, take_vert, 0), (26.0, take_stats, 0),
        (36.0 + 3 * last, gather_sums, 1), (38.85 + 3 * last, send_total_y, 1),
        (41.5 + 3 * last, send_total_c, 1), (43.5 + 3 * last, send_total_outer, 1),
        (1000.0, finish_out, 0), (1001.0, finish_sums, 1),
    ]
    prepare()
    for _, stage, j in sorted(plan, key=lambda entry: entry[0]):
        stage(j)

    for j in range(chunks):
        for copy in one(j) + two(j) + three(j, y, x) + four(j, y, x):
            copy.wait_send()

        def sent_outer(p, carry):
            outer_copy(j, p, lev).wait_send()
            return carry

        lax.fori_loop(1, outer, sent_outer, 0)

        @pl.when(lev != keeper(j))
        def _():
            outer_copy(j, 0, lev).wait_send()

        @pl.when(lev == keeper(j))
        def _():
            def sent(p, carry):
                lifted_copy(j, p, h).wait_send()
                raised_copy(j, p, h).wait_send()
                return carry

            raised_copy(j, 0, h).wait_send()
            lax.fori_loop(1, outer, sent, 0)

    for k in range(2):
        for copy in (total_x(k), total_y(k), total_c(k)):
            copy.wait_send()

        def sent_total(p, carry):
            total_outer(k, p).wait_send()
            return carry

        lax.fori_loop(1, outer, sent_total, 0)
    vert_copy(lev).wait_send()


def per_device(perturbations, gradient, horizontal, area, vertical):
    members, levels, columns = perturbations.shape
    vectors = gradient.shape[0]
    modes = horizontal.shape[0]
    n = lax.axis_size("col")
    sizes = (members, levels, vectors, modes, columns)
    chunks = modes * vectors // LANES
    tiles = max(2, -(-members // n))
    rows = tiles * levels
    outer = n // 4
    most = (tiles + 1) // 2 * levels
    f32 = jnp.float32
    vmem = pl.BlockSpec(memory_space=pltpu.VMEM)
    dma = pltpu.SemaphoreType.DMA

    held = chunks * n * rows * LANES * 4 * 9 // 2
    limit = min(60 * 2**20, held + 20 * 2**20)
    increment, background = pl.pallas_call(
        functools.partial(kernel, sizes, n),
        out_shape=(
            jax.ShapeDtypeStruct((vectors, levels, columns), f32),
            jax.ShapeDtypeStruct((8, LANES), f32),
        ),
        in_specs=[pl.BlockSpec(memory_space=pltpu.HBM)] * 5,
        out_specs=(vmem, vmem),
        scratch_shapes=[
            pltpu.VMEM((members, levels, columns), f32),
            pltpu.VMEM((vectors, levels, columns), f32),
            pltpu.VMEM((modes, columns), f32),
            pltpu.VMEM((1, columns), f32),
            pltpu.VMEM((levels, vertical.shape[0]), f32),
            pltpu.VMEM((levels, 2 * members, columns), jnp.bfloat16),
            pltpu.VMEM((levels, vectors, columns), f32),
            pltpu.VMEM((levels, vectors, columns), f32),
            pltpu.VMEM((chunks, outer, 2, 2, rows, LANES), f32),
            pltpu.VMEM((chunks, outer, 2, most, LANES), f32),
            pltpu.VMEM((chunks, outer, 2, most, LANES), f32),
            pltpu.VMEM((chunks, outer, rows, LANES), f32),
            pltpu.VMEM((chunks, 2, outer, rows, LANES), f32),
            pltpu.VMEM((chunks, rows, LANES), f32),
            pltpu.VMEM((chunks, outer, 2, 2, rows, LANES), f32),
            pltpu.VMEM((2, 6 + outer, 8, LANES), f32),
            pltpu.VMEM((2, levels, LANES), f32),
            pltpu.VMEM((8, LANES), f32),
            pltpu.VMEM((8, LANES), f32),
            pltpu.VMEM((modes, columns), f32),
            dma((2, BLOCKS)), dma((3,)),
            dma((chunks, 8)), dma((chunks, 8)),
            dma((chunks, outer)), dma((chunks, 2, outer)),
            dma((chunks, outer)), dma((chunks, outer)),
            dma((chunks, outer)), dma((chunks, outer)),
            dma((2, 6 + outer)), dma((2, 6 + outer)),
            dma((1,)), dma((1,)),
        ],
        compiler_params=pltpu.CompilerParams(
            collective_id=0, has_side_effects=True, vmem_limit_bytes=limit
        ),
        name="covariance",
    )(*(
        pltpu.with_memory_space_constraint(array, pltpu.HBM)
        for array in (perturbations, gradient, horizontal, area.reshape(1, columns), vertical.T)
    ))
    return increment, background[0, :vectors]


def solution(mesh):
    return jax.shard_map(
        per_device,
        mesh=mesh,
        in_specs=(
            P(None, "lev", "col"),
            P(None, "lev", "col"),
            P(None, "col"),
            P("col"),
            P(None, "lev"),
        ),
        out_specs=(P(None, "lev", "col"), P()),
        check_vma=False,
    )
```

```python
import functools

import jax
import jax.numpy as jnp
from jax import lax
from jax.experimental import pallas as pl
from jax.experimental.pallas import tpu as pltpu
from jax.sharding import PartitionSpec as P

LANES = 128
NT = (((1,), (1,)), ((), ()))
TN = (((0,), (0,)), ((), ()))
NN = (((1,), (0,)), ((), ()))
UNROLL = 8
BLOCKS = 4


def split(x):
    high = x.astype(jnp.bfloat16)
    low = (x - high.astype(jnp.float32)).astype(jnp.bfloat16)
    return high, low


def exact_dot(a, b, dims):
    return lax.dot_general(
        a, b, dims, precision=lax.Precision.HIGHEST, preferred_element_type=jnp.float32
    )


def timetable(*stages):
    starts = (3.5, 8.3, 12.8, 17.0, 22.9, 29.1, 32.5, 40.7)
    paces = (2.05, 2.4, 2.7, 2.6, 2.9, 2.9, 3.0, 2.3)
    return zip(stages, starts, paces)


def kernel(
    sizes, n, pert_hbm, grad_hbm, hor_hbm, area_hbm, vert_hbm, out_ref, bg_ref,
    pert_ref, grad_ref, hor_ref, area_ref, vert_ref,
    halves, weighted, acc, terms, first_a, first_b, second, third, raised, lifted,
    near, far_z, plane_a, plane_b, totals, verticals, sums, weights, scaled,
    load_p, load_s, send_h, recv_h, send_g, recv_g, send_l, recv_l, send_m, recv_m,
    send_t, recv_t, send_v, recv_v,
):
    members, levels, vectors, modes, columns = sizes
    group = LANES // vectors
    chunks = modes // group
    vmodes = vert_ref.shape[1]
    rows = terms.shape[4]
    tiles = rows // levels
    outer = n // 4
    used = members * levels
    me = lax.axis_index("col")
    lev = lax.axis_index("lev")
    other = 1 - lev
    x = lax.rem(me, 2)
    y = lax.rem(lax.div(me, 2), 2)
    h = lax.div(me, 4)
    not_x, not_y = 1 - x, 1 - y
    x_peer = (4 * h + 2 * y + not_x, lev)
    y_peer = (4 * h + 2 * not_y + x, lev)
    partner = (me, other)
    mesh_id = pl.DeviceIdType.MESH
    barrier = pltpu.get_barrier_semaphore()

    def along(p):
        return 4 * lax.rem(h + p, outer) + 2 * y + x

    def greet(device):
        pl.semaphore_signal(barrier, inc=1, device_id=device, device_id_type=mesh_id)

    def greet_outer(p, carry):
        greet((along(p), lev))
        greet((along(p), other))
        return carry

    for device in (x_peer, y_peer, partner):
        greet(device)
    lax.fori_loop(1, outer, greet_outer, 0)

    wide_block = columns // BLOCKS

    def load_block(q):
        part = pl.ds(q * wide_block, wide_block)
        return (
            pltpu.make_async_copy(
                pert_hbm.at[:, :, part], pert_ref.at[:, :, part], load_p.at[0, q]
            ),
            pltpu.make_async_copy(
                grad_hbm.at[:, :, part], grad_ref.at[:, :, part], load_p.at[1, q]
            ),
        )

    small = [
        pltpu.make_async_copy(source, target, load_s.at[i])
        for i, (source, target) in enumerate(
            ((area_hbm, area_ref), (hor_hbm, hor_ref), (vert_hbm, vert_ref))
        )
    ]
    for copy in small:
        copy.start()
    for q in range(BLOCKS):
        for copy in load_block(q):
            copy.start()

    def remote(src, dst, send, recv, device):
        return pltpu.make_async_remote_copy(
            src_ref=src, dst_ref=dst, send_sem=send, recv_sem=recv,
            device_id=device, device_id_type=mesh_id,
        )

    def halfway(j):
        count = (tiles + 1 - j % 2) // 2 * levels
        return pl.ds(0, count), pl.ds(count, rows - count), count, rows - count

    def half_copy(j, i, src, dst, device):
        return remote(src, dst, send_h.at[j, i], recv_h.at[j, i], device)

    def one(j):
        a, b, na, nb = halfway(j)
        return (
            half_copy(j, 0, terms.at[j, :, :, not_x, a], first_a.at[j, :, :, pl.ds(0, na)], x_peer),
            half_copy(j, 1, terms.at[j, :, not_y, :, b], first_b.at[j, :, :, pl.ds(0, nb)], y_peer),
        )

    def two(j):
        a, b, na, nb = halfway(j)
        return (
            half_copy(j, 2, first_a.at[j, :, not_y, pl.ds(0, na)], second.at[j, :, a], y_peer),
            half_copy(j, 3, first_b.at[j, :, not_x, pl.ds(0, nb)], second.at[j, :, b], x_peer),
        )

    def keeper(j):
        return j % 2

    z_first = outer == 4
    low_bit, high_bit = lax.rem(h, 2), lax.div(h, 2)
    z_near = (4 * (2 * high_bit + 1 - low_bit) + 2 * y + x, lev)
    z_far = (4 * (2 * (1 - high_bit) + low_bit) + 2 * y + x, lev)

    def paired(ref):
        return ref.at[0].reshape(2, 2, 2, 2, rows, LANES)

    def near_copy():
        return half_copy(0, 0, paired(terms).at[:, 1 - low_bit], near, z_near)

    def far_copy():
        return half_copy(0, 1, near.at[1 - high_bit], far_z, z_far)

    def plane_one():
        a, b, na, nb = halfway(0)
        return (
            half_copy(0, 2, far_z.at[:, not_x, a], plane_a, x_peer),
            half_copy(0, 3, far_z.at[not_y, :, b], plane_b, y_peer),
        )

    def plane_two():
        a, b, na, nb = halfway(0)
        return (
            half_copy(0, 4, plane_a.at[not_y], second.at[0, 0, a], y_peer),
            half_copy(0, 5, plane_b.at[not_x], second.at[0, 0, b], x_peer),
        )

    def own_copy():
        return remote(
            second.at[0, 0], third.at[0, lev, 0], send_g.at[0, 0], recv_g.at[0, lev, 0], partner
        )

    def own_arrival():
        return remote(
            second.at[0, 0], third.at[0, other, 0], send_g.at[0, 0], recv_g.at[0, other, 0], partner
        )

    def back_one(yy, xx):
        a, b, _, _ = halfway(0)
        block_a = lifted.at[0, h, yy, x, a]
        block_b = lifted.at[0, h, y, xx, b]
        return (
            half_copy(0, 6, block_a, block_a, y_peer),
            half_copy(0, 7, block_b, block_b, x_peer),
        )

    def back_two(yy, xx):
        a, b, _, _ = halfway(0)
        block_a = lifted.at[0, h, :, xx, a]
        block_b = lifted.at[0, h, yy, :, b]
        return (
            half_copy(0, 8, block_a, block_a, x_peer),
            half_copy(0, 9, block_b, block_b, y_peer),
        )

    def back_far(slot):
        block = lifted.at[0, slot]
        return half_copy(0, 10, block, block, z_far)

    def back_near(bit):
        block = paired(lifted).at[:, bit]
        return half_copy(0, 11, block, block, z_near)

    def outer_copy(j, p, source):
        return remote(
            second.at[j, lax.rem(h + p, outer)], third.at[j, source, p],
            send_g.at[j, p], recv_g.at[j, source, p], (along(p), keeper(j)),
        )

    def lifted_copy(j, p, slot):
        block = lifted.at[j, slot, y, x]
        return remote(block, block, send_l.at[j, p], recv_l.at[j, p], (along(p), lev))

    def raised_copy(j, p, slot):
        return remote(
            raised.at[j], lifted.at[j, slot, y, x],
            send_m.at[j, p], recv_m.at[j, p], (along(p), other),
        )

    def three(j, yy, xx):
        a, b, _, _ = halfway(j)
        block_a = lifted.at[j, :, yy, x, a]
        block_b = lifted.at[j, :, y, xx, b]
        return (
            half_copy(j, 4, block_a, block_a, y_peer),
            half_copy(j, 5, block_b, block_b, x_peer),
        )

    def four(j, yy, xx):
        a, b, _, _ = halfway(j)
        block_a = lifted.at[j, :, :, xx, a]
        block_b = lifted.at[j, :, yy, :, b]
        return (
            half_copy(j, 6, block_a, block_a, x_peer),
            half_copy(j, 7, block_b, block_b, y_peer),
        )

    def vert_copy(slot):
        block = verticals.at[slot]
        return remote(block, block, send_v.at[0], recv_v.at[0], partner)

    def total_copy(k, source, target, device):
        return remote(
            totals.at[k, source], totals.at[k, target],
            send_t.at[k, target], recv_t.at[k, target], device,
        )

    def total_outer(k, p):
        return total_copy(k, 6, 6 + p, (along(p), lev))

    def total_x(k):
        return total_copy(k, 0, 1, x_peer)

    def total_y(k):
        return total_copy(k, 2, 3, y_peer)

    def total_c(k):
        return total_copy(k, 4, 5, partner)

    def send_total_x(k):
        total_x(k).start()

    def send_total_y(k):
        total_x(k).wait_recv()
        totals[k, 2] = totals[k, 0] + totals[k, 1]
        total_y(k).start()

    def send_total_c(k):
        total_y(k).wait_recv()
        totals[k, 4] = totals[k, 2] + totals[k, 3]
        total_c(k).start()

    def send_total_outer(k):
        total_c(k).wait_recv()
        totals[k, 6] = totals[k, 4] + totals[k, 5]

        def send(p, carry):
            total_outer(k, p).start()
            return carry

        lax.fori_loop(1, outer, send, 0)

    def take_total(k):
        def take(p, carry):
            total_outer(k, p).wait_recv()
            return carry + totals[k, 6 + p]

        return lax.fori_loop(1, outer, take, totals[k, 6])

    lane = lax.broadcasted_iota(jnp.int32, (modes, LANES), 1)
    row = lax.broadcasted_iota(jnp.int32, (modes, LANES), 0)
    sums[...] = jnp.zeros(sums.shape, jnp.float32)
    verticals[lev] = jnp.zeros(verticals.shape[1:], jnp.float32)
    if used < n * rows:
        for j in range(chunks):
            flat = terms.at[j].reshape(n * rows, LANES)
            flat[used:, :] = jnp.zeros((n * rows - used, LANES), jnp.float32)
    for copy in small:
        copy.wait()
    area = area_ref[...]
    verticals[lev, :, :vmodes] = vert_ref[...]

    def prepare():
        for q in range(BLOCKS):
            for copy in load_block(q):
                copy.wait()
            for c in range(q * wide_block, (q + 1) * wide_block, LANES):
                lanes = slice(c, c + LANES)
                for k in range(0, members, 16):
                    high, low = split(jnp.swapaxes(pert_ref[k : k + 16, :, lanes], 0, 1))
                    halves[:, k : k + 16, lanes] = high
                    halves[:, members + k : members + k + 16, lanes] = low
                for v in range(0, vectors, 8):
                    block = jnp.swapaxes(grad_ref[v : v + 8, :, lanes], 0, 1)
                    weighted[:, v : v + 8, lanes] = block * area[:, lanes]

    def statistics():
        power = jnp.sum(area * hor_ref[...] * hor_ref[...], axis=1, keepdims=True)
        powers = jnp.sum(
            jnp.where(lane == row, jnp.broadcast_to(power, (modes, LANES)), 0.0),
            axis=0, keepdims=True,
        )
        total = jnp.broadcast_to(jnp.sum(area, axis=1, keepdims=True), (1, LANES))
        stat_row = jnp.where(lane[:1] == modes, total, powers)
        totals[0, 0] = jnp.broadcast_to(stat_row, totals.shape[2:])

    def over_levels(step):
        def body(i, carry):
            for u in range(UNROLL):
                step(i * UNROLL + u)
            return carry

        lax.fori_loop(0, levels // UNROLL, body, 0)

    def adjoint(j):
        flat = terms.at[j].reshape(n * rows, LANES)

        def step(l):
            base = weighted[l]
            products = jnp.concatenate(
                [base * hor_ref[b : b + 1, :] for b in range(j * group, (j + 1) * group)],
                axis=0,
            )
            both = jnp.concatenate(split(products), axis=0)
            out = lax.dot_general(halves[l], both, NT, preferred_element_type=jnp.float32)
            flat[pl.ds(l, members, stride=levels), :] = out[:members, :LANES] + (
                out[members:, :LANES] + out[:members, LANES:]
            )

        over_levels(step)

    def send_one(j):
        for copy in one(j):
            copy.start()

    def send_two(j):
        a, b, na, nb = halfway(j)
        one_a, one_b = one(j)
        two_a, two_b = two(j)

        def add_a(i, carry):
            first_a[j, i, not_y, :na] += terms[j, i, not_y, x, a]
            return carry

        def add_b(i, carry):
            first_b[j, i, not_x, :nb] += terms[j, i, y, not_x, b]
            return carry

        one_a.wait_recv()
        lax.fori_loop(0, outer, add_a, 0)
        two_a.start()
        one_b.wait_recv()
        lax.fori_loop(0, outer, add_b, 0)
        two_b.start()

    def z_start(j):
        near_copy().start()

    def z_middle(j):
        near_copy().wait_recv()
        mine = paired(terms)
        for i in range(2):
            near[i] += mine[i, low_bit]
        far_copy().start()

    def z_end(j):
        a, b, na, nb = halfway(0)
        far_copy().wait_recv()
        far_z[...] += near[high_bit]
        for copy in plane_one():
            copy.start()

    def z_plane(j):
        a, b, na, nb = halfway(0)
        one_a, one_b = plane_one()
        two_a, two_b = plane_two()
        one_a.wait_recv()
        plane_a[not_y] += far_z[not_y, x, a]
        two_a.start()
        one_b.wait_recv()
        plane_b[not_x] += far_z[y, not_x, b]
        two_b.start()

    def z_own(j):
        a, b, na, nb = halfway(0)
        for copy in plane_two():
            copy.wait_recv()
        second[0, 0, a] += far_z[y, x, a] + plane_a[y]
        second[0, 0, b] += far_z[y, x, b] + plane_b[x]

        @pl.when(lev != keeper(0))
        def _():
            own_copy().start()

    def z_back(j):
        @pl.when(lev != keeper(0))
        def _():
            raised_copy(0, 0, h).wait_recv()

        for copy in back_one(y, x):
            copy.start()

    def z_back_plane(j):
        one_a, one_b = back_one(not_y, not_x)
        two_a, two_b = back_two(y, x)
        one_a.wait_recv()
        two_a.start()
        one_b.wait_recv()
        two_b.start()

    def z_back_far(j):
        for copy in back_two(not_y, not_x):
            copy.wait_recv()
        back_far(h).start()

    def z_back_near(j):
        back_far(2 * (1 - high_bit) + low_bit).wait_recv()
        back_near(low_bit).start()

    def add_second(j, there):
        a, b, na, nb = halfway(j)
        second[j, there, a] += terms[j, there, y, x, a] + first_a[j, there, y, :na]
        second[j, there, b] += terms[j, there, y, x, b] + first_b[j, there, x, :nb]

    def send_three(j):
        for copy in two(j):
            copy.wait_recv()

        def send_outer(p, carry):
            add_second(j, lax.rem(h + p, outer))
            outer_copy(j, p, lev).start()
            return carry

        lax.fori_loop(1, outer, send_outer, 0)
        add_second(j, h)

        @pl.when(lev != keeper(j))
        def _():
            outer_copy(j, 0, lev).start()

    def mix(j):
        @pl.when(lev == keeper(j))
        def _():
            direct = z_first and j == 0
            mine = 0 if direct else h

            def take(p, carry):
                outer_copy(j, p, lev).wait_recv()
                second[j, h] += third[j, lev, p]
                outer_copy(j, p, other).wait_recv()
                third[j, other, 0] += third[j, other, p]
                return carry

            if direct:
                own_arrival().wait_recv()
            else:
                outer_copy(j, 0, other).wait_recv()
                lax.fori_loop(1, outer, take, 0)

            def wide(block):
                return jnp.concatenate(
                    [block[i * levels : (i + 1) * levels] for i in range(tiles)], axis=1
                )

            far = verticals[other][:, :vmodes]
            control = exact_dot(vert_ref[...], wide(second[j, mine]), TN) + exact_dot(
                far, wide(third[j, other, 0]), TN
            )
            near_lifted = exact_dot(vert_ref[...], control, NN)
            far_lifted = exact_dot(far, control, NN)
            square = jnp.zeros((1, LANES), jnp.float32)
            for i in range(tiles):
                lanes = slice(i * LANES, (i + 1) * LANES)
                part = slice(i * levels, (i + 1) * levels)
                lifted[j, h, y, x, part, :] = near_lifted[:, lanes]
                raised[j, part, :] = far_lifted[:, lanes]
                square = square + jnp.sum(
                    control[:, lanes] * control[:, lanes], axis=0, keepdims=True
                )
            sums[j : j + 1, :] = square

            def start_lifted(p, carry):
                lifted_copy(j, p, h).start()
                raised_copy(j, p, h).start()
                return carry

            raised_copy(j, 0, h).start()
            if not direct:
                lax.fori_loop(1, outer, start_lifted, 0)

    def send_g2(j):
        @pl.when(lev == keeper(j))
        def _():
            def take(p, carry):
                lifted_copy(j, p, lax.rem(h + outer - p, outer)).wait_recv()
                return carry

            lax.fori_loop(1, outer, take, 0)

        @pl.when(lev != keeper(j))
        def _():
            def take(p, carry):
                raised_copy(j, p, lax.rem(h + outer - p, outer)).wait_recv()
                return carry

            lax.fori_loop(0, outer, take, 0)

        for copy in three(j, y, x):
            copy.start()

    def send_g3(j):
        three_a, three_b = three(j, not_y, not_x)
        four_a, four_b = four(j, y, x)
        three_a.wait_recv()
        four_a.start()
        three_b.wait_recv()
        four_b.start()

    def forward(j):
        if z_first and j == 0:
            back_near(1 - low_bit).wait_recv()
        else:
            for copy in four(j, not_y, not_x):
                copy.wait_recv()
        flat = lifted.at[j].reshape(n * rows, LANES)
        width = 256

        def step(l):
            high, low = split(flat[pl.ds(l, members, stride=levels), :])
            lhs = jnp.concatenate([high, high, low], axis=0)
            for c in range(0, columns, width):
                cols = slice(c, c + width)
                rhs = jnp.concatenate([halves[l, :, cols], halves[l, :members, cols]], axis=0)
                spread = lax.dot_general(lhs, rhs, TN, preferred_element_type=jnp.float32)
                value = None if j == 0 else acc[l, :, cols]
                for g in range(group):
                    b = j * group + g
                    term = spread[g * vectors : (g + 1) * vectors] * scaled[b : b + 1, cols]
                    value = term if value is None else value + term
                acc[l, :, cols] = value

        over_levels(step)

    def take_stats(k):
        stat = 0.5 * take_total(k)
        spread = jnp.broadcast_to(stat[:1], (modes, LANES))
        power = jnp.sum(jnp.where(lane == row, spread, 0.0), axis=1, keepdims=True)
        whole = jnp.sum(jnp.where(lane == modes, spread, 0.0), axis=1, keepdims=True)
        factor = 1.0 / jnp.sqrt(modes * (power / whole + 1e-06))
        scale = factor * (columns * n / whole)
        scaled[...] = hor_ref[...] * (factor * scale)
        placed = jnp.where(
            lax.div(lane, vectors) == lax.rem(row, group),
            jnp.broadcast_to(scale, lane.shape), 0.0,
        )
        for j in range(chunks):
            weights[j : j + 1, :] = jnp.sum(
                placed[j * group : (j + 1) * group], axis=0, keepdims=True
            )

    def gather_sums(k):
        part = jnp.zeros((1, LANES), jnp.float32)
        for j in range(chunks):
            weight = weights[j : j + 1, :]
            part = part + sums[j : j + 1, :] * weight * weight
        totals[k, 0] = jnp.broadcast_to(part, totals.shape[2:])
        send_total_x(k)

    def finish_sums(k):
        part = take_total(k)
        folded = part
        for g in range(1, group):
            folded = folded + pltpu.roll(part, g * vectors, 1)
        bg_ref[...] = 0.5 * folded

    def meet(k):
        pl.semaphore_wait(barrier, 3 + 2 * (outer - 1))
        vert_copy(lev).start()

    def take_vert(k):
        vert_copy(other).wait_recv()

    def set_stats(k):
        statistics()
        send_total_x(k)

    def finish_out(k):
        for c in range(0, columns, LANES):
            lanes = slice(c, c + LANES)
            for v in range(0, vectors, 8):
                out_ref[v : v + 8, :, lanes] = jnp.swapaxes(acc[:, v : v + 8, lanes], 0, 1)

    shift = 1 if z_first else 0
    plan = []
    for index, (stage, start, pace) in enumerate(
        timetable(adjoint, send_one, send_two, send_three, mix, send_g2, send_g3, forward)
    ):
        for j in range(0 if index in (0, 7) else shift, chunks):
            plan.append((start + pace * (j if index in (0, 7) else j - shift), stage, j))
    if z_first:
        plan += [
            (6.9, z_start, 0), (12.5, z_middle, 0), (16.8, z_end, 0), (18.5, z_plane, 0),
            (20.5, z_own, 0), (22.5, mix, 0), (24.5, z_back, 0), (26.5, z_back_plane, 0),
            (28.5, z_back_far, 0), (32.4, z_back_near, 0),
        ]
    last = chunks - 5
    plan += [
        (6.8, meet, 0), (8.65, set_stats, 0), (13.0, send_total_y, 0), (16.7, send_total_c, 0),
        (19.0, send_total_outer, 0), (20.0, take_vert, 0), (26.0, take_stats, 0),
        (36.0 + 3 * last, gather_sums, 1), (38.85 + 3 * last, send_total_y, 1),
        (41.5 + 3 * last, send_total_c, 1), (43.5 + 3 * last, send_total_outer, 1),
        (1000.0, finish_out, 0), (1001.0, finish_sums, 1),
    ]
    prepare()
    for _, stage, j in sorted(plan, key=lambda entry: entry[0]):
        stage(j)

    if z_first:
        for copy in (
            (near_copy(), far_copy(), back_far(h), back_near(low_bit))
            + plane_one() + plane_two() + back_one(y, x) + back_two(y, x)
        ):
            copy.wait_send()

        @pl.when(lev != keeper(0))
        def _():
            own_copy().wait_send()

        @pl.when(lev == keeper(0))
        def _():
            raised_copy(0, 0, h).wait_send()

    for j in range(shift, chunks):
        for copy in one(j) + two(j) + three(j, y, x) + four(j, y, x):
            copy.wait_send()

        def sent_outer(p, carry):
            outer_copy(j, p, lev).wait_send()
            return carry

        lax.fori_loop(1, outer, sent_outer, 0)

        @pl.when(lev != keeper(j))
        def _():
            outer_copy(j, 0, lev).wait_send()

        @pl.when(lev == keeper(j))
        def _():
            def sent(p, carry):
                lifted_copy(j, p, h).wait_send()
                raised_copy(j, p, h).wait_send()
                return carry

            raised_copy(j, 0, h).wait_send()
            lax.fori_loop(1, outer, sent, 0)

    for k in range(2):
        for copy in (total_x(k), total_y(k), total_c(k)):
            copy.wait_send()

        def sent_total(p, carry):
            total_outer(k, p).wait_send()
            return carry

        lax.fori_loop(1, outer, sent_total, 0)
    vert_copy(lev).wait_send()


def per_device(perturbations, gradient, horizontal, area, vertical):
    members, levels, columns = perturbations.shape
    vectors = gradient.shape[0]
    modes = horizontal.shape[0]
    n = lax.axis_size("col")
    sizes = (members, levels, vectors, modes, columns)
    chunks = modes * vectors // LANES
    tiles = max(2, -(-members // n))
    rows = tiles * levels
    outer = n // 4
    most = (tiles + 1) // 2 * levels
    f32 = jnp.float32
    vmem = pl.BlockSpec(memory_space=pltpu.VMEM)
    dma = pltpu.SemaphoreType.DMA

    held = chunks * n * rows * LANES * 4 * 9 // 2
    limit = min(60 * 2**20, held + 20 * 2**20)
    increment, background = pl.pallas_call(
        functools.partial(kernel, sizes, n),
        out_shape=(
            jax.ShapeDtypeStruct((vectors, levels, columns), f32),
            jax.ShapeDtypeStruct((8, LANES), f32),
        ),
        in_specs=[pl.BlockSpec(memory_space=pltpu.HBM)] * 5,
        out_specs=(vmem, vmem),
        scratch_shapes=[
            pltpu.VMEM((members, levels, columns), f32),
            pltpu.VMEM((vectors, levels, columns), f32),
            pltpu.VMEM((modes, columns), f32),
            pltpu.VMEM((1, columns), f32),
            pltpu.VMEM((levels, vertical.shape[0]), f32),
            pltpu.VMEM((levels, 2 * members, columns), jnp.bfloat16),
            pltpu.VMEM((levels, vectors, columns), f32),
            pltpu.VMEM((levels, vectors, columns), f32),
            pltpu.VMEM((chunks, outer, 2, 2, rows, LANES), f32),
            pltpu.VMEM((chunks, outer, 2, most, LANES), f32),
            pltpu.VMEM((chunks, outer, 2, most, LANES), f32),
            pltpu.VMEM((chunks, outer, rows, LANES), f32),
            pltpu.VMEM((chunks, 2, outer, rows, LANES), f32),
            pltpu.VMEM((chunks, rows, LANES), f32),
            pltpu.VMEM((chunks, outer, 2, 2, rows, LANES), f32),
            pltpu.VMEM((2, 2, 2, rows, LANES), f32),
            pltpu.VMEM((2, 2, rows, LANES), f32),
            pltpu.VMEM((2, most, LANES), f32),
            pltpu.VMEM((2, rows - most, LANES), f32),
            pltpu.VMEM((2, 6 + outer, 8, LANES), f32),
            pltpu.VMEM((2, levels, LANES), f32),
            pltpu.VMEM((8, LANES), f32),
            pltpu.VMEM((8, LANES), f32),
            pltpu.VMEM((modes, columns), f32),
            dma((2, BLOCKS)), dma((3,)),
            dma((chunks, 12)), dma((chunks, 12)),
            dma((chunks, outer)), dma((chunks, 2, outer)),
            dma((chunks, outer)), dma((chunks, outer)),
            dma((chunks, outer)), dma((chunks, outer)),
            dma((2, 6 + outer)), dma((2, 6 + outer)),
            dma((1,)), dma((1,)),
        ],
        compiler_params=pltpu.CompilerParams(
            collective_id=0, has_side_effects=True, vmem_limit_bytes=limit
        ),
        name="covariance",
    )(*(
        pltpu.with_memory_space_constraint(array, pltpu.HBM)
        for array in (perturbations, gradient, horizontal, area.reshape(1, columns), vertical.T)
    ))
    return increment, background[0, :vectors]


def solution(mesh):
    return jax.shard_map(
        per_device,
        mesh=mesh,
        in_specs=(
            P(None, "lev", "col"),
            P(None, "lev", "col"),
            P(None, "col"),
            P("col"),
            P(None, "lev"),
        ),
        out_specs=(P(None, "lev", "col"), P()),
        check_vma=False,
    )
```

```python
import functools

import jax
import jax.numpy as jnp
from jax import lax
from jax.experimental import pallas as pl
from jax.experimental.pallas import tpu as pltpu
from jax.sharding import PartitionSpec as P

LANES = 128
NT = (((1,), (1,)), ((), ()))
TN = (((0,), (0,)), ((), ()))
NN = (((1,), (0,)), ((), ()))
UNROLL = 8
BLOCKS = 4


def split(x):
    high = x.astype(jnp.bfloat16)
    low = (x - high.astype(jnp.float32)).astype(jnp.bfloat16)
    return high, low


def exact_dot(a, b, dims):
    return lax.dot_general(
        a, b, dims, precision=lax.Precision.HIGHEST, preferred_element_type=jnp.float32
    )


PLAN = (
    0, 800, 100, 101, 3, 107, 106, 900, 1, 103, 201, 102, 2, 200,
    206, 207, 104, 105, 301, 4, 203, 300, 202, 108, 1000, 307, 306, 109,
    1300, 401, 204, 205, 302, 1100, 303, 400, 208, 407, 501, 304, 305, 406,
    209, 402, 500, 308, 507, 309, 1200, 404, 405, 506, 403, 502, 607, 600,
    408, 409, 601, 606, 1400, 504, 1501, 505, 503, 602, 508, 1001, 605, 509,
    604, 603, 703, 608, 1101, 1201, 609, 700, 702, 701, 704, 1600, 1701,
)


def order(chunks, stages):
    if chunks == 5:
        entries = [(entry // 100, entry % 100) for entry in PLAN]
    else:
        starts = (0, 5, 10, 16, 22, 28, 34, 40)
        timed = [(start + 2.8 * j, k, j) for k, start in enumerate(starts) if k in (0, 7) for j in range(chunks)]
        timed += [
            (start + 1.4 * i, k, i)
            for k, start in enumerate(starts) if k not in (0, 7) for i in range(2 * chunks)
        ]
        late = 22 + 2.8 * chunks
        timed += [
            (4.9, 8, 0), (4.95, 9, 0), (12, 10, 0), (16, 11, 0), (18, 12, 0), (21, 13, 0),
            (late, 14, 0), (late + 1, 15, 1), (late + 4, 10, 1), (late + 7, 11, 1),
            (late + 9, 12, 1), (1e6, 16, 0), (2e6, 17, 1),
        ]
        entries = [entry[1:] for entry in sorted(timed)]
    return [(stages[k], i) for k, i in entries]


def kernel(
    sizes, n, pert_hbm, grad_hbm, hor_hbm, area_hbm, vert_hbm, out_ref, bg_ref,
    pert_ref, grad_ref, hor_ref, area_ref, vert_ref,
    halves, weighted, acc, terms, first, second, third, raised, lifted,
    totals, verticals, sums, weights, scaled,
    load_p, load_s, send_h, recv_h, send_g, recv_g, send_l, recv_l,
    send_t, recv_t, send_v, recv_v,
):
    members, levels, vectors, modes, columns = sizes
    group = LANES // vectors
    chunks = modes // group
    vmodes = vert_ref.shape[1]
    rows = terms.shape[4]
    tiles = rows // levels
    outer = n // 4
    used = members * levels
    me = lax.axis_index("col")
    lev = lax.axis_index("lev")
    other = 1 - lev
    x = lax.rem(me, 2)
    y = lax.rem(lax.div(me, 2), 2)
    h = lax.div(me, 4)
    not_x, not_y = 1 - x, 1 - y
    x_peer = (4 * h + 2 * y + not_x, lev)
    y_peer = (4 * h + 2 * not_y + x, lev)
    partner = (me, other)
    mesh_id = pl.DeviceIdType.MESH
    barrier = pltpu.get_barrier_semaphore()

    def along(p):
        return 4 * lax.rem(h + p, outer) + 2 * y + x

    def greet(device):
        pl.semaphore_signal(barrier, inc=1, device_id=device, device_id_type=mesh_id)

    def greet_outer(p, carry):
        greet((along(p), lev))
        greet((along(p), other))
        return carry

    for device in (x_peer, y_peer, partner):
        greet(device)
    lax.fori_loop(1, outer, greet_outer, 0)

    wide_block = columns // BLOCKS

    def load_block(q):
        part = pl.ds(q * wide_block, wide_block)
        return (
            pltpu.make_async_copy(
                pert_hbm.at[:, :, part], pert_ref.at[:, :, part], load_p.at[0, q]
            ),
            pltpu.make_async_copy(
                grad_hbm.at[:, :, part], grad_ref.at[:, :, part], load_p.at[1, q]
            ),
        )

    small = [
        pltpu.make_async_copy(source, target, load_s.at[i])
        for i, (source, target) in enumerate(
            ((area_hbm, area_ref), (hor_hbm, hor_ref), (vert_hbm, vert_ref))
        )
    ]
    for copy in small:
        copy.start()
    for q in range(BLOCKS):
        for copy in load_block(q):
            copy.start()

    def remote(src, dst, send, recv, device):
        return pltpu.make_async_remote_copy(
            src_ref=src, dst_ref=dst, send_sem=send, recv_sem=recv,
            device_id=device, device_id_type=mesh_id,
        )

    def piece(i):
        j, side = i // 2, i % 2
        count = (tiles + 1 - j % 2) // 2 * levels
        start, size = (0, count) if side == 0 else (count, rows - count)
        return j, side, pl.ds(start, size), size

    def half_copy(i, k, src, dst, device):
        return remote(src, dst, send_h.at[i, k], recv_h.at[i, k], device)

    def one(i):
        j, side, span, size = piece(i)
        target = first.at[i, :, :, pl.ds(0, size)]
        if side == 0:
            return half_copy(i, 0, terms.at[j, :, :, not_x, span], target, x_peer)
        return half_copy(i, 0, terms.at[j, :, not_y, :, span], target, y_peer)

    def two(i):
        j, side, span, size = piece(i)
        index, device = (not_y, y_peer) if side == 0 else (not_x, x_peer)
        source = first.at[i, :, index, pl.ds(0, size)]
        return half_copy(i, 1, source, second.at[j, :, span], device)

    def keeper(i):
        return i % 2

    def outer_copy(i, p, source):
        j, side, span, size = piece(i)
        return remote(
            second.at[j, lax.rem(h + p, outer), span], third.at[j, source, p, span],
            send_g.at[i, p], recv_g.at[i, source, p], (along(p), keeper(i)),
        )

    def lifted_copy(i, p, slot):
        j, side, span, size = piece(i)
        block = lifted.at[j, slot, y, x, span]
        return remote(block, block, send_l.at[i, p], recv_l.at[i, p], (along(p), lev))

    def raised_copy(i, p, slot):
        j, side, span, size = piece(i)
        return remote(
            raised.at[j, span], lifted.at[j, slot, y, x, span],
            send_g.at[i, p], recv_l.at[i, p], (along(p), other),
        )

    def three(i, yy, xx):
        j, side, span, size = piece(i)
        if side == 0:
            block = lifted.at[j, :, yy, x, span]
            return half_copy(i, 2, block, block, y_peer)
        block = lifted.at[j, :, y, xx, span]
        return half_copy(i, 2, block, block, x_peer)

    def four(i, yy, xx):
        j, side, span, size = piece(i)
        if side == 0:
            block = lifted.at[j, :, :, xx, span]
            return half_copy(i, 3, block, block, x_peer)
        block = lifted.at[j, :, yy, :, span]
        return half_copy(i, 3, block, block, y_peer)

    def vert_copy(slot):
        block = verticals.at[slot]
        return remote(block, block, send_v.at[0], recv_v.at[0], partner)

    def total_copy(k, source, target, device):
        return remote(
            totals.at[k, source], totals.at[k, target],
            send_t.at[k, target], recv_t.at[k, target], device,
        )

    def total_outer(k, p):
        return total_copy(k, 6, 6 + p, (along(p), lev))

    def total_x(k):
        return total_copy(k, 0, 1, x_peer)

    def total_y(k):
        return total_copy(k, 2, 3, y_peer)

    def total_c(k):
        return total_copy(k, 4, 5, partner)

    def send_total_x(k):
        total_x(k).start()

    def send_total_y(k):
        total_x(k).wait_recv()
        totals[k, 2] = totals[k, 0] + totals[k, 1]
        total_y(k).start()

    def send_total_c(k):
        total_y(k).wait_recv()
        totals[k, 4] = totals[k, 2] + totals[k, 3]
        total_c(k).start()

    def send_total_outer(k):
        total_c(k).wait_recv()
        totals[k, 6] = totals[k, 4] + totals[k, 5]

        def send(p, carry):
            total_outer(k, p).start()
            return carry

        lax.fori_loop(1, outer, send, 0)

    def take_total(k):
        def take(p, carry):
            total_outer(k, p).wait_recv()
            return carry + totals[k, 6 + p]

        return lax.fori_loop(1, outer, take, totals[k, 6])

    lane = lax.broadcasted_iota(jnp.int32, (modes, LANES), 1)
    row = lax.broadcasted_iota(jnp.int32, (modes, LANES), 0)
    sums[...] = jnp.zeros(sums.shape, jnp.float32)
    verticals[lev] = jnp.zeros(verticals.shape[1:], jnp.float32)
    if used < n * rows:
        for j in range(chunks):
            flat = terms.at[j].reshape(n * rows, LANES)
            flat[used:, :] = jnp.zeros((n * rows - used, LANES), jnp.float32)
    for copy in small:
        copy.wait()
    area = area_ref[...]
    verticals[lev, :, :vmodes] = vert_ref[...]

    def prepare():
        for q in range(BLOCKS):
            for copy in load_block(q):
                copy.wait()
            for c in range(q * wide_block, (q + 1) * wide_block, LANES):
                lanes = slice(c, c + LANES)
                for k in range(0, members, 16):
                    high, low = split(jnp.swapaxes(pert_ref[k : k + 16, :, lanes], 0, 1))
                    halves[:, k : k + 16, lanes] = high
                    halves[:, members + k : members + k + 16, lanes] = low
                for v in range(0, vectors, 8):
                    block = jnp.swapaxes(grad_ref[v : v + 8, :, lanes], 0, 1)
                    weighted[:, v : v + 8, lanes] = block * area[:, lanes]

    def statistics():
        power = jnp.sum(area * hor_ref[...] * hor_ref[...], axis=1, keepdims=True)
        powers = jnp.sum(
            jnp.where(lane == row, jnp.broadcast_to(power, (modes, LANES)), 0.0),
            axis=0, keepdims=True,
        )
        total = jnp.broadcast_to(jnp.sum(area, axis=1, keepdims=True), (1, LANES))
        stat_row = jnp.where(lane[:1] == modes, total, powers)
        totals[0, 0] = jnp.broadcast_to(stat_row, totals.shape[2:])

    def over_levels(step):
        def body(i, carry):
            for u in range(UNROLL):
                step(i * UNROLL + u)
            return carry

        lax.fori_loop(0, levels // UNROLL, body, 0)

    def adjoint(j):
        flat = terms.at[j].reshape(n * rows, LANES)

        def step(l):
            base = weighted[l]
            products = jnp.concatenate(
                [base * hor_ref[b : b + 1, :] for b in range(j * group, (j + 1) * group)],
                axis=0,
            )
            both = jnp.concatenate(split(products), axis=0)
            out = lax.dot_general(halves[l], both, NT, preferred_element_type=jnp.float32)
            flat[pl.ds(l, members, stride=levels), :] = out[:members, :LANES] + (
                out[members:, :LANES] + out[:members, LANES:]
            )

        over_levels(step)

    def send_one(i):
        one(i).start()

    def send_two(i):
        j, side, span, size = piece(i)
        one(i).wait_recv()

        def add(q, carry):
            if side == 0:
                first[i, q, not_y, :size] += terms[j, q, not_y, x, span]
            else:
                first[i, q, not_x, :size] += terms[j, q, y, not_x, span]
            return carry

        lax.fori_loop(0, outer, add, 0)
        two(i).start()

    def send_three(i):
        j, side, span, size = piece(i)
        two(i).wait_recv()

        def add_second(there):
            mine = first[i, there, y if side == 0 else x, :size]
            second[j, there, span] += terms[j, there, y, x, span] + mine

        def send_outer(p, carry):
            add_second(lax.rem(h + p, outer))
            outer_copy(i, p, lev).start()
            return carry

        lax.fori_loop(1, outer, send_outer, 0)
        add_second(h)

        @pl.when(lev != keeper(i))
        def _():
            outer_copy(i, 0, lev).start()

    def mix(i):
        j, side, span, size = piece(i)

        @pl.when(lev == keeper(i))
        def _():
            def take(p, carry):
                outer_copy(i, p, lev).wait_send()
                outer_copy(i, p, lev).wait_recv()
                second[j, h, span] += third[j, lev, p, span]
                outer_copy(i, p, other).wait_recv()
                third[j, other, 0, span] += third[j, other, p, span]
                return carry

            outer_copy(i, 0, other).wait_recv()
            lax.fori_loop(1, outer, take, 0)

            def wide(block):
                return jnp.concatenate(
                    [block[t : t + levels] for t in range(0, size, levels)], axis=1
                )

            far = verticals[other][:, :vmodes]
            control = exact_dot(vert_ref[...], wide(second[j, h, span]), TN) + exact_dot(
                far, wide(third[j, other, 0, span]), TN
            )
            near_lifted = exact_dot(vert_ref[...], control, NN)
            far_lifted = exact_dot(far, control, NN)
            square = jnp.zeros((1, LANES), jnp.float32)
            for t in range(size // levels):
                lanes = slice(t * LANES, (t + 1) * LANES)
                part = pl.ds(span.start + t * levels, levels)
                lifted[j, h, y, x, part, :] = near_lifted[:, lanes]
                raised[j, part, :] = far_lifted[:, lanes]
                square = square + jnp.sum(
                    control[:, lanes] * control[:, lanes], axis=0, keepdims=True
                )
            sums[j : j + 1, :] = sums[j : j + 1, :] + square

            def start_lifted(p, carry):
                lifted_copy(i, p, h).start()
                raised_copy(i, p, h).start()
                return carry

            raised_copy(i, 0, h).start()
            lax.fori_loop(1, outer, start_lifted, 0)

    def send_g2(i):
        @pl.when(lev == keeper(i))
        def _():
            def take(p, carry):
                lifted_copy(i, p, lax.rem(h + outer - p, outer)).wait_recv()
                return carry

            lax.fori_loop(1, outer, take, 0)

        @pl.when(lev != keeper(i))
        def _():
            def take(p, carry):
                raised_copy(i, p, lax.rem(h + outer - p, outer)).wait_recv()
                return carry

            lax.fori_loop(0, outer, take, 0)

        three(i, y, x).start()

    def send_g3(i):
        three(i, not_y, not_x).wait_recv()
        four(i, y, x).start()

    started = []

    def forward(j):
        fresh = not started
        started.append(j)
        for i in (2 * j, 2 * j + 1):
            four(i, not_y, not_x).wait_recv()
        flat = lifted.at[j].reshape(n * rows, LANES)
        width = 256

        def step(l):
            high, low = split(flat[pl.ds(l, members, stride=levels), :])
            lhs = jnp.concatenate([high, high, low], axis=0)
            for c in range(0, columns, width):
                cols = slice(c, c + width)
                rhs = jnp.concatenate([halves[l, :, cols], halves[l, :members, cols]], axis=0)
                spread = lax.dot_general(lhs, rhs, TN, preferred_element_type=jnp.float32)
                value = None if fresh else acc[l, :, cols]
                for g in range(group):
                    b = j * group + g
                    term = spread[g * vectors : (g + 1) * vectors] * scaled[b : b + 1, cols]
                    value = term if value is None else value + term
                acc[l, :, cols] = value

        over_levels(step)

    def take_stats(k):
        stat = 0.5 * take_total(k)
        spread = jnp.broadcast_to(stat[:1], (modes, LANES))
        power = jnp.sum(jnp.where(lane == row, spread, 0.0), axis=1, keepdims=True)
        whole = jnp.sum(jnp.where(lane == modes, spread, 0.0), axis=1, keepdims=True)
        factor = 1.0 / jnp.sqrt(modes * (power / whole + 1e-06))
        scale = factor * (columns * n / whole)
        scaled[...] = hor_ref[...] * (factor * scale)
        placed = jnp.where(
            lax.div(lane, vectors) == lax.rem(row, group),
            jnp.broadcast_to(scale, lane.shape), 0.0,
        )
        for j in range(chunks):
            weights[j : j + 1, :] = jnp.sum(
                placed[j * group : (j + 1) * group], axis=0, keepdims=True
            )

    def gather_sums(k):
        part = jnp.zeros((1, LANES), jnp.float32)
        for j in range(chunks):
            weight = weights[j : j + 1, :]
            part = part + sums[j : j + 1, :] * weight * weight
        totals[k, 0] = jnp.broadcast_to(part, totals.shape[2:])
        send_total_x(k)

    def finish_sums(k):
        part = take_total(k)
        folded = part
        for g in range(1, group):
            folded = folded + pltpu.roll(part, g * vectors, 1)
        bg_ref[...] = 0.5 * folded

    def meet(k):
        pl.semaphore_wait(barrier, 3 + 2 * (outer - 1))
        vert_copy(lev).start()

    def take_vert(k):
        vert_copy(other).wait_recv()

    def set_stats(k):
        statistics()
        send_total_x(k)

    def finish_out(k):
        for c in range(0, columns, LANES):
            lanes = slice(c, c + LANES)
            for v in range(0, vectors, 8):
                out_ref[v : v + 8, :, lanes] = jnp.swapaxes(acc[:, v : v + 8, lanes], 0, 1)

    prepare()
    for stage, i in order(chunks, (
        adjoint, send_one, send_two, send_three, mix, send_g2, send_g3, forward, meet, set_stats,
        send_total_y, send_total_c, send_total_outer, take_vert, take_stats, gather_sums,
        finish_out, finish_sums,
    )):
        stage(i)

    for i in range(2 * chunks):
        for copy in (one(i), two(i), three(i, y, x), four(i, y, x)):
            copy.wait_send()

        @pl.when(lev != keeper(i))
        def _():
            def sent(p, carry):
                outer_copy(i, p, lev).wait_send()
                return carry

            lax.fori_loop(0, outer, sent, 0)

        @pl.when(lev == keeper(i))
        def _():
            def sent(p, carry):
                lifted_copy(i, p, h).wait_send()
                raised_copy(i, p, h).wait_send()
                return carry

            raised_copy(i, 0, h).wait_send()
            lax.fori_loop(1, outer, sent, 0)

    for k in range(2):
        for copy in (total_x(k), total_y(k), total_c(k)):
            copy.wait_send()

        def sent_total(p, carry):
            total_outer(k, p).wait_send()
            return carry

        lax.fori_loop(1, outer, sent_total, 0)
    vert_copy(lev).wait_send()


def per_device(perturbations, gradient, horizontal, area, vertical):
    members, levels, columns = perturbations.shape
    vectors = gradient.shape[0]
    modes = horizontal.shape[0]
    n = lax.axis_size("col")
    sizes = (members, levels, vectors, modes, columns)
    chunks = modes * vectors // LANES
    tiles = max(2, -(-members // n))
    rows = tiles * levels
    outer = n // 4
    most = (tiles + 1) // 2 * levels
    f32 = jnp.float32
    vmem = pl.BlockSpec(memory_space=pltpu.VMEM)
    dma = pltpu.SemaphoreType.DMA

    held = chunks * n * rows * LANES * 4 * 9 // 2
    limit = min(60 * 2**20, held + 20 * 2**20)
    increment, background = pl.pallas_call(
        functools.partial(kernel, sizes, n),
        out_shape=(
            jax.ShapeDtypeStruct((vectors, levels, columns), f32),
            jax.ShapeDtypeStruct((8, LANES), f32),
        ),
        in_specs=[pl.BlockSpec(memory_space=pltpu.HBM)] * 5,
        out_specs=(vmem, vmem),
        scratch_shapes=[
            pltpu.VMEM((members, levels, columns), f32),
            pltpu.VMEM((vectors, levels, columns), f32),
            pltpu.VMEM((modes, columns), f32),
            pltpu.VMEM((1, columns), f32),
            pltpu.VMEM((levels, vertical.shape[0]), f32),
            pltpu.VMEM((levels, 2 * members, columns), jnp.bfloat16),
            pltpu.VMEM((levels, vectors, columns), f32),
            pltpu.VMEM((levels, vectors, columns), f32),
            pltpu.VMEM((chunks, outer, 2, 2, rows, LANES), f32),
            pltpu.VMEM((2 * chunks, outer, 2, most, LANES), f32),
            pltpu.VMEM((chunks, outer, rows, LANES), f32),
            pltpu.VMEM((chunks, 2, outer, rows, LANES), f32),
            pltpu.VMEM((chunks, rows, LANES), f32),
            pltpu.VMEM((chunks, outer, 2, 2, rows, LANES), f32),
            pltpu.VMEM((2, 6 + outer, 8, LANES), f32),
            pltpu.VMEM((2, levels, LANES), f32),
            pltpu.VMEM((8, LANES), f32),
            pltpu.VMEM((8, LANES), f32),
            pltpu.VMEM((modes, columns), f32),
            dma((2, BLOCKS)), dma((3,)),
            dma((2 * chunks, 4)), dma((2 * chunks, 4)),
            dma((2 * chunks, outer)), dma((2 * chunks, 2, outer)),
            dma((2 * chunks, outer)), dma((2 * chunks, outer)),
            dma((2, 6 + outer)), dma((2, 6 + outer)),
            dma((1,)), dma((1,)),
        ],
        compiler_params=pltpu.CompilerParams(
            collective_id=0, has_side_effects=True, vmem_limit_bytes=limit
        ),
        name="covariance",
    )(*(
        pltpu.with_memory_space_constraint(array, pltpu.HBM)
        for array in (perturbations, gradient, horizontal, area.reshape(1, columns), vertical.T)
    ))
    return increment, background[0, :vectors]


def solution(mesh):
    return jax.shard_map(
        per_device,
        mesh=mesh,
        in_specs=(
            P(None, "lev", "col"),
            P(None, "lev", "col"),
            P(None, "col"),
            P("col"),
            P(None, "lev"),
        ),
        out_specs=(P(None, "lev", "col"), P()),
        check_vma=False,
    )
```

```python
import functools

import jax
import jax.numpy as jnp
from jax import lax
from jax.experimental import pallas as pl
from jax.experimental.pallas import tpu as pltpu
from jax.sharding import PartitionSpec as P

LANES = 128
NT = (((1,), (1,)), ((), ()))
TN = (((0,), (0,)), ((), ()))
NN = (((1,), (0,)), ((), ()))
UNROLL = 8
BLOCKS = 4
Z_FIRST = (0, 3)


def split(x):
    high = x.astype(jnp.bfloat16)
    low = (x - high.astype(jnp.float32)).astype(jnp.bfloat16)
    return high, low


def exact_dot(a, b, dims):
    return lax.dot_general(
        a, b, dims, precision=lax.Precision.HIGHEST, preferred_element_type=jnp.float32
    )


PLAN = (
    1, 800, 102, 103, 3, 107, 106, 2, 105, 104, 0, 100, 202, 101,
    900, 206, 207, 4, 108, 1000, 204, 302, 203, 109, 205, 307, 201, 306,
    1100, 304, 303, 208, 1200, 200, 305, 209, 301, 1300, 402, 407, 1803, 300,
    308, 403, 309, 406, 503, 404, 1800, 401, 502, 400, 405, 603, 1400, 500,
    507, 408, 409, 602, 506, 504, 1903, 1501, 600, 501, 607, 505, 606, 508,
    1001, 509, 604, 601, 1900, 605, 608, 609, 703, 1101, 1201, 701, 702, 704,
    700, 1600, 1701,
)


def order(chunks, stages):
    if chunks == 5:
        entries = [(entry // 100, entry % 100) for entry in PLAN]
    else:
        starts = (0, 5, 10, 16, 22, 28, 34, 40)
        timed = [(start + 2.8 * j, k, j) for k, start in enumerate(starts) if k in (0, 7) for j in range(chunks)]
        timed += [
            (start + 1.4 * i, k, i)
            for k, start in enumerate(starts) if k not in (0, 7) for i in range(2 * chunks)
        ]
        timed += [(start + 1.4 * i, k, i) for k, start in ((18, 19), (19, 37)) for i in Z_FIRST]
        late = 22 + 2.8 * chunks
        timed += [
            (4.9, 8, 0), (4.95, 9, 0), (12, 10, 0), (16, 11, 0), (18, 12, 0), (21, 13, 0),
            (late, 14, 0), (late + 1, 15, 1), (late + 4, 10, 1), (late + 7, 11, 1),
            (late + 9, 12, 1), (1e6, 16, 0), (2e6, 17, 1),
        ]
        entries = [entry[1:] for entry in sorted(timed)]
    return [(stages[k], i) for k, i in entries]


def kernel(
    sizes, n, pert_hbm, grad_hbm, hor_hbm, area_hbm, vert_hbm, out_ref, bg_ref,
    pert_ref, grad_ref, hor_ref, area_ref, vert_ref,
    halves, weighted, acc, terms, first, second, third, raised, lifted,
    z_in, z_sum, plane, totals, verticals, sums, weights, scaled,
    load_p, load_s, send_h, recv_h, send_g, recv_g, send_l, recv_l,
    send_t, recv_t, send_v, recv_v,
):
    members, levels, vectors, modes, columns = sizes
    group = LANES // vectors
    chunks = modes // group
    vmodes = vert_ref.shape[1]
    rows = terms.shape[4]
    tiles = rows // levels
    outer = n // 4
    used = members * levels
    me = lax.axis_index("col")
    lev = lax.axis_index("lev")
    other = 1 - lev
    x = lax.rem(me, 2)
    y = lax.rem(lax.div(me, 2), 2)
    h = lax.div(me, 4)
    not_x, not_y = 1 - x, 1 - y
    x_peer = (4 * h + 2 * y + not_x, lev)
    y_peer = (4 * h + 2 * not_y + x, lev)
    partner = (me, other)
    mesh_id = pl.DeviceIdType.MESH
    barrier = pltpu.get_barrier_semaphore()

    def along(p):
        return 4 * lax.rem(h + p, outer) + 2 * y + x

    def greet(device):
        pl.semaphore_signal(barrier, inc=1, device_id=device, device_id_type=mesh_id)

    def greet_outer(p, carry):
        greet((along(p), lev))
        greet((along(p), other))
        return carry

    for device in (x_peer, y_peer, partner):
        greet(device)
    lax.fori_loop(1, outer, greet_outer, 0)

    wide_block = columns // BLOCKS

    def load_block(q):
        part = pl.ds(q * wide_block, wide_block)
        return (
            pltpu.make_async_copy(
                pert_hbm.at[:, :, part], pert_ref.at[:, :, part], load_p.at[0, q]
            ),
            pltpu.make_async_copy(
                grad_hbm.at[:, :, part], grad_ref.at[:, :, part], load_p.at[1, q]
            ),
        )

    small = [
        pltpu.make_async_copy(source, target, load_s.at[i])
        for i, (source, target) in enumerate(
            ((area_hbm, area_ref), (hor_hbm, hor_ref), (vert_hbm, vert_ref))
        )
    ]
    for copy in small:
        copy.start()
    for q in range(BLOCKS):
        for copy in load_block(q):
            copy.start()

    def remote(src, dst, send, recv, device):
        return pltpu.make_async_remote_copy(
            src_ref=src, dst_ref=dst, send_sem=send, recv_sem=recv,
            device_id=device, device_id_type=mesh_id,
        )

    def piece(i):
        j, side = i // 2, i % 2
        count = (tiles + 1 - j % 2) // 2 * levels
        start, size = (0, count) if side == 0 else (count, rows - count)
        return j, side, pl.ds(start, size), size

    def half_copy(i, k, src, dst, device):
        return remote(src, dst, send_h.at[i, k], recv_h.at[i, k], device)

    def one(i):
        j, side, span, size = piece(i)
        target = first.at[i, :, :, pl.ds(0, size)]
        if side == 0:
            return half_copy(i, 0, terms.at[j, :, :, not_x, span], target, x_peer)
        return half_copy(i, 0, terms.at[j, :, not_y, :, span], target, y_peer)

    def two(i):
        j, side, span, size = piece(i)
        index, device = (not_y, y_peer) if side == 0 else (not_x, x_peer)
        source = first.at[i, :, index, pl.ds(0, size)]
        return half_copy(i, 1, source, second.at[j, :, span], device)

    def keeper(i):
        return i % 2

    def z_copy(i, p):
        j, side, span, size = piece(i)
        return remote(
            terms.at[j, lax.rem(h + p, outer), :, :, span],
            z_in.at[Z_FIRST.index(i), p, :, :, pl.ds(0, size)],
            send_g.at[i, p], recv_g.at[i, lev, p], (along(p), lev),
        )

    def plane_one(i):
        j, side, span, size = piece(i)
        k = Z_FIRST.index(i)
        source = z_sum.at[k, :, not_x] if side == 0 else z_sum.at[k, not_y]
        rows_ = pl.ds(0, size)
        source = source.at[:, rows_]
        target = plane.at[k, :, rows_]
        return half_copy(i, 0, source, target, x_peer if side == 0 else y_peer)

    def plane_two(i):
        j, side, span, size = piece(i)
        index, device = (not_y, y_peer) if side == 0 else (not_x, x_peer)
        source = plane.at[Z_FIRST.index(i), index, pl.ds(0, size)]
        return half_copy(i, 1, source, second.at[j, h, span], device)

    def back_one(i, yy, xx):
        j, side, span, size = piece(i)
        if side == 0:
            block = lifted.at[j, h, yy, x, span]
            return half_copy(i, 2, block, block, y_peer)
        block = lifted.at[j, h, y, xx, span]
        return half_copy(i, 2, block, block, x_peer)

    def back_two(i, yy, xx):
        j, side, span, size = piece(i)
        if side == 0:
            block = lifted.at[j, h, :, xx, span]
            return half_copy(i, 3, block, block, x_peer)
        block = lifted.at[j, h, yy, :, span]
        return half_copy(i, 3, block, block, y_peer)

    def back_z(i, p, slot):
        j, side, span, size = piece(i)
        block = lifted.at[j, slot, :, :, span]
        return remote(block, block, send_l.at[i, p], recv_l.at[i, p], (along(p), lev))

    def each_outer(step):
        def body(p, carry):
            step(p)
            return carry

        lax.fori_loop(1, outer, body, 0)

    def outer_copy(i, p, source):
        j, side, span, size = piece(i)
        return remote(
            second.at[j, lax.rem(h + p, outer), span], third.at[j, source, p, span],
            send_g.at[i, p], recv_g.at[i, source, p], (along(p), keeper(i)),
        )

    def lifted_copy(i, p, slot):
        j, side, span, size = piece(i)
        block = lifted.at[j, slot, y, x, span]
        return remote(block, block, send_l.at[i, p], recv_l.at[i, p], (along(p), lev))

    def raised_copy(i, p, slot):
        j, side, span, size = piece(i)
        return remote(
            raised.at[j, span], lifted.at[j, slot, y, x, span],
            send_g.at[i, p], recv_l.at[i, p], (along(p), other),
        )

    def three(i, yy, xx):
        j, side, span, size = piece(i)
        if side == 0:
            block = lifted.at[j, :, yy, x, span]
            return half_copy(i, 2, block, block, y_peer)
        block = lifted.at[j, :, y, xx, span]
        return half_copy(i, 2, block, block, x_peer)

    def four(i, yy, xx):
        j, side, span, size = piece(i)
        if side == 0:
            block = lifted.at[j, :, :, xx, span]
            return half_copy(i, 3, block, block, x_peer)
        block = lifted.at[j, :, yy, :, span]
        return half_copy(i, 3, block, block, y_peer)

    def vert_copy(slot):
        block = verticals.at[slot]
        return remote(block, block, send_v.at[0], recv_v.at[0], partner)

    def total_copy(k, source, target, device):
        return remote(
            totals.at[k, source], totals.at[k, target],
            send_t.at[k, target], recv_t.at[k, target], device,
        )

    def total_outer(k, p):
        return total_copy(k, 6, 6 + p, (along(p), lev))

    def total_x(k):
        return total_copy(k, 0, 1, x_peer)

    def total_y(k):
        return total_copy(k, 2, 3, y_peer)

    def total_c(k):
        return total_copy(k, 4, 5, partner)

    def send_total_x(k):
        total_x(k).start()

    def send_total_y(k):
        total_x(k).wait_recv()
        totals[k, 2] = totals[k, 0] + totals[k, 1]
        total_y(k).start()

    def send_total_c(k):
        total_y(k).wait_recv()
        totals[k, 4] = totals[k, 2] + totals[k, 3]
        total_c(k).start()

    def send_total_outer(k):
        total_c(k).wait_recv()
        totals[k, 6] = totals[k, 4] + totals[k, 5]

        def send(p, carry):
            total_outer(k, p).start()
            return carry

        lax.fori_loop(1, outer, send, 0)

    def take_total(k):
        def take(p, carry):
            total_outer(k, p).wait_recv()
            return carry + totals[k, 6 + p]

        return lax.fori_loop(1, outer, take, totals[k, 6])

    lane = lax.broadcasted_iota(jnp.int32, (modes, LANES), 1)
    row = lax.broadcasted_iota(jnp.int32, (modes, LANES), 0)
    sums[...] = jnp.zeros(sums.shape, jnp.float32)
    verticals[lev] = jnp.zeros(verticals.shape[1:], jnp.float32)
    if used < n * rows:
        for j in range(chunks):
            flat = terms.at[j].reshape(n * rows, LANES)
            flat[used:, :] = jnp.zeros((n * rows - used, LANES), jnp.float32)
    for copy in small:
        copy.wait()
    area = area_ref[...]
    verticals[lev, :, :vmodes] = vert_ref[...]

    def prepare():
        for q in range(BLOCKS):
            for copy in load_block(q):
                copy.wait()
            for c in range(q * wide_block, (q + 1) * wide_block, LANES):
                lanes = slice(c, c + LANES)
                for k in range(0, members, 16):
                    high, low = split(jnp.swapaxes(pert_ref[k : k + 16, :, lanes], 0, 1))
                    halves[:, k : k + 16, lanes] = high
                    halves[:, members + k : members + k + 16, lanes] = low
                for v in range(0, vectors, 8):
                    block = jnp.swapaxes(grad_ref[v : v + 8, :, lanes], 0, 1)
                    weighted[:, v : v + 8, lanes] = block * area[:, lanes]

    def statistics():
        power = jnp.sum(area * hor_ref[...] * hor_ref[...], axis=1, keepdims=True)
        powers = jnp.sum(
            jnp.where(lane == row, jnp.broadcast_to(power, (modes, LANES)), 0.0),
            axis=0, keepdims=True,
        )
        total = jnp.broadcast_to(jnp.sum(area, axis=1, keepdims=True), (1, LANES))
        stat_row = jnp.where(lane[:1] == modes, total, powers)
        totals[0, 0] = jnp.broadcast_to(stat_row, totals.shape[2:])

    def over_levels(step):
        def body(i, carry):
            for u in range(UNROLL):
                step(i * UNROLL + u)
            return carry

        lax.fori_loop(0, levels // UNROLL, body, 0)

    def adjoint(j):
        flat = terms.at[j].reshape(n * rows, LANES)

        def step(l):
            base = weighted[l]
            products = jnp.concatenate(
                [base * hor_ref[b : b + 1, :] for b in range(j * group, (j + 1) * group)],
                axis=0,
            )
            both = jnp.concatenate(split(products), axis=0)
            out = lax.dot_general(halves[l], both, NT, preferred_element_type=jnp.float32)
            flat[pl.ds(l, members, stride=levels), :] = out[:members, :LANES] + (
                out[members:, :LANES] + out[:members, LANES:]
            )

        over_levels(step)

    def send_one(i):
        if i in Z_FIRST:
            each_outer(lambda p: z_copy(i, p).start())
        else:
            one(i).start()

    def send_two(i):
        j, side, span, size = piece(i)
        if i in Z_FIRST:
            k = Z_FIRST.index(i)
            z_sum[k, :, :, :size] = terms[j, h, :, :, span]

            def take(p):
                z_copy(i, p).wait_recv()
                z_sum[k, :, :, :size] += z_in[k, p, :, :, :size]

            each_outer(take)
            plane_one(i).start()
            return
        one(i).wait_recv()

        def add(q, carry):
            if side == 0:
                first[i, q, not_y, :size] += terms[j, q, not_y, x, span]
            else:
                first[i, q, not_x, :size] += terms[j, q, y, not_x, span]
            return carry

        lax.fori_loop(0, outer, add, 0)
        two(i).start()

    def send_three(i):
        j, side, span, size = piece(i)
        if i in Z_FIRST:
            k = Z_FIRST.index(i)
            plane_one(i).wait_recv()
            if side == 0:
                plane[k, not_y, :size] += z_sum[k, not_y, x, :size]
            else:
                plane[k, not_x, :size] += z_sum[k, y, not_x, :size]
            plane_two(i).start()
            return
        two(i).wait_recv()

        def add_second(there):
            mine = first[i, there, y if side == 0 else x, :size]
            second[j, there, span] += terms[j, there, y, x, span] + mine

        def send_outer(p, carry):
            add_second(lax.rem(h + p, outer))
            outer_copy(i, p, lev).start()
            return carry

        lax.fori_loop(1, outer, send_outer, 0)
        add_second(h)

        @pl.when(lev != keeper(i))
        def _():
            outer_copy(i, 0, lev).start()

    def z_own(i):
        j, side, span, size = piece(i)
        k = Z_FIRST.index(i)
        plane_two(i).wait_recv()
        second[j, h, span] += z_sum[k, y, x, :size] + plane[k, y if side == 0 else x, :size]

        @pl.when(lev != keeper(i))
        def _():
            outer_copy(i, 0, lev).start()

    def mix(i):
        j, side, span, size = piece(i)

        @pl.when(lev == keeper(i))
        def _():
            def take(p, carry):
                outer_copy(i, p, lev).wait_send()
                outer_copy(i, p, lev).wait_recv()
                second[j, h, span] += third[j, lev, p, span]
                outer_copy(i, p, other).wait_recv()
                third[j, other, 0, span] += third[j, other, p, span]
                return carry

            outer_copy(i, 0, other).wait_recv()
            if i not in Z_FIRST:
                lax.fori_loop(1, outer, take, 0)

            def wide(block):
                return jnp.concatenate(
                    [block[t : t + levels] for t in range(0, size, levels)], axis=1
                )

            far = verticals[other][:, :vmodes]
            control = exact_dot(vert_ref[...], wide(second[j, h, span]), TN) + exact_dot(
                far, wide(third[j, other, 0, span]), TN
            )
            near_lifted = exact_dot(vert_ref[...], control, NN)
            far_lifted = exact_dot(far, control, NN)
            square = jnp.zeros((1, LANES), jnp.float32)
            for t in range(size // levels):
                lanes = slice(t * LANES, (t + 1) * LANES)
                part = pl.ds(span.start + t * levels, levels)
                lifted[j, h, y, x, part, :] = near_lifted[:, lanes]
                raised[j, part, :] = far_lifted[:, lanes]
                square = square + jnp.sum(
                    control[:, lanes] * control[:, lanes], axis=0, keepdims=True
                )
            sums[j : j + 1, :] = sums[j : j + 1, :] + square

            def start_lifted(p, carry):
                lifted_copy(i, p, h).start()
                raised_copy(i, p, h).start()
                return carry

            raised_copy(i, 0, h).start()
            if i not in Z_FIRST:
                lax.fori_loop(1, outer, start_lifted, 0)

    def send_g2(i):
        if i in Z_FIRST:
            @pl.when(lev != keeper(i))
            def _():
                raised_copy(i, 0, h).wait_recv()

            back_one(i, y, x).start()
            return

        @pl.when(lev == keeper(i))
        def _():
            def take(p, carry):
                lifted_copy(i, p, lax.rem(h + outer - p, outer)).wait_recv()
                return carry

            lax.fori_loop(1, outer, take, 0)

        @pl.when(lev != keeper(i))
        def _():
            def take(p, carry):
                raised_copy(i, p, lax.rem(h + outer - p, outer)).wait_recv()
                return carry

            lax.fori_loop(0, outer, take, 0)

        three(i, y, x).start()

    def send_g3(i):
        if i in Z_FIRST:
            back_one(i, not_y, not_x).wait_recv()
            back_two(i, y, x).start()
        else:
            three(i, not_y, not_x).wait_recv()
            four(i, y, x).start()

    def send_g4(i):
        back_two(i, not_y, not_x).wait_recv()
        each_outer(lambda p: back_z(i, p, h).start())

    started = []

    def forward(j):
        fresh = not started
        started.append(j)
        for i in (2 * j, 2 * j + 1):
            if i in Z_FIRST:
                each_outer(lambda p: back_z(i, p, lax.rem(h + outer - p, outer)).wait_recv())
            else:
                four(i, not_y, not_x).wait_recv()
        flat = lifted.at[j].reshape(n * rows, LANES)
        width = 256

        def step(l):
            high, low = split(flat[pl.ds(l, members, stride=levels), :])
            lhs = jnp.concatenate([high, high, low], axis=0)
            for c in range(0, columns, width):
                cols = slice(c, c + width)
                rhs = jnp.concatenate([halves[l, :, cols], halves[l, :members, cols]], axis=0)
                spread = lax.dot_general(lhs, rhs, TN, preferred_element_type=jnp.float32)
                value = None if fresh else acc[l, :, cols]
                for g in range(group):
                    b = j * group + g
                    term = spread[g * vectors : (g + 1) * vectors] * scaled[b : b + 1, cols]
                    value = term if value is None else value + term
                acc[l, :, cols] = value

        over_levels(step)

    def take_stats(k):
        stat = 0.5 * take_total(k)
        spread = jnp.broadcast_to(stat[:1], (modes, LANES))
        power = jnp.sum(jnp.where(lane == row, spread, 0.0), axis=1, keepdims=True)
        whole = jnp.sum(jnp.where(lane == modes, spread, 0.0), axis=1, keepdims=True)
        factor = 1.0 / jnp.sqrt(modes * (power / whole + 1e-06))
        scale = factor * (columns * n / whole)
        scaled[...] = hor_ref[...] * (factor * scale)
        placed = jnp.where(
            lax.div(lane, vectors) == lax.rem(row, group),
            jnp.broadcast_to(scale, lane.shape), 0.0,
        )
        for j in range(chunks):
            weights[j : j + 1, :] = jnp.sum(
                placed[j * group : (j + 1) * group], axis=0, keepdims=True
            )

    def gather_sums(k):
        part = jnp.zeros((1, LANES), jnp.float32)
        for j in range(chunks):
            weight = weights[j : j + 1, :]
            part = part + sums[j : j + 1, :] * weight * weight
        totals[k, 0] = jnp.broadcast_to(part, totals.shape[2:])
        send_total_x(k)

    def finish_sums(k):
        part = take_total(k)
        folded = part
        for g in range(1, group):
            folded = folded + pltpu.roll(part, g * vectors, 1)
        bg_ref[...] = 0.5 * folded

    def meet(k):
        pl.semaphore_wait(barrier, 3 + 2 * (outer - 1))
        vert_copy(lev).start()

    def take_vert(k):
        vert_copy(other).wait_recv()

    def set_stats(k):
        statistics()
        send_total_x(k)

    def finish_out(k):
        for c in range(0, columns, LANES):
            lanes = slice(c, c + LANES)
            for v in range(0, vectors, 8):
                out_ref[v : v + 8, :, lanes] = jnp.swapaxes(acc[:, v : v + 8, lanes], 0, 1)

    prepare()
    for stage, i in order(chunks, (
        adjoint, send_one, send_two, send_three, mix, send_g2, send_g3, forward, meet, set_stats,
        send_total_y, send_total_c, send_total_outer, take_vert, take_stats, gather_sums,
        finish_out, finish_sums, z_own, send_g4,
    )):
        stage(i)

    for i in range(2 * chunks):
        if i in Z_FIRST:
            for copy in (plane_one(i), plane_two(i), back_one(i, y, x), back_two(i, y, x)):
                copy.wait_send()
            each_outer(lambda p: z_copy(i, p).wait_send())
            each_outer(lambda p: back_z(i, p, h).wait_send())

            @pl.when(lev != keeper(i))
            def _():
                outer_copy(i, 0, lev).wait_send()

            @pl.when(lev == keeper(i))
            def _():
                raised_copy(i, 0, h).wait_send()

            continue
        for copy in (one(i), two(i), three(i, y, x), four(i, y, x)):
            copy.wait_send()

        @pl.when(lev != keeper(i))
        def _():
            def sent(p, carry):
                outer_copy(i, p, lev).wait_send()
                return carry

            lax.fori_loop(0, outer, sent, 0)

        @pl.when(lev == keeper(i))
        def _():
            def sent(p, carry):
                lifted_copy(i, p, h).wait_send()
                raised_copy(i, p, h).wait_send()
                return carry

            raised_copy(i, 0, h).wait_send()
            lax.fori_loop(1, outer, sent, 0)

    for k in range(2):
        for copy in (total_x(k), total_y(k), total_c(k)):
            copy.wait_send()

        def sent_total(p, carry):
            total_outer(k, p).wait_send()
            return carry

        lax.fori_loop(1, outer, sent_total, 0)
    vert_copy(lev).wait_send()


def per_device(perturbations, gradient, horizontal, area, vertical):
    members, levels, columns = perturbations.shape
    vectors = gradient.shape[0]
    modes = horizontal.shape[0]
    n = lax.axis_size("col")
    sizes = (members, levels, vectors, modes, columns)
    chunks = modes * vectors // LANES
    tiles = max(2, -(-members // n))
    rows = tiles * levels
    outer = n // 4
    most = (tiles + 1) // 2 * levels
    f32 = jnp.float32
    vmem = pl.BlockSpec(memory_space=pltpu.VMEM)
    dma = pltpu.SemaphoreType.DMA

    held = chunks * n * rows * LANES * 4 * 9 // 2
    limit = min(60 * 2**20, held + 20 * 2**20)
    increment, background = pl.pallas_call(
        functools.partial(kernel, sizes, n),
        out_shape=(
            jax.ShapeDtypeStruct((vectors, levels, columns), f32),
            jax.ShapeDtypeStruct((8, LANES), f32),
        ),
        in_specs=[pl.BlockSpec(memory_space=pltpu.HBM)] * 5,
        out_specs=(vmem, vmem),
        scratch_shapes=[
            pltpu.VMEM((members, levels, columns), f32),
            pltpu.VMEM((vectors, levels, columns), f32),
            pltpu.VMEM((modes, columns), f32),
            pltpu.VMEM((1, columns), f32),
            pltpu.VMEM((levels, vertical.shape[0]), f32),
            pltpu.VMEM((levels, 2 * members, columns), jnp.bfloat16),
            pltpu.VMEM((levels, vectors, columns), f32),
            pltpu.VMEM((levels, vectors, columns), f32),
            pltpu.VMEM((chunks, outer, 2, 2, rows, LANES), f32),
            pltpu.VMEM((2 * chunks, outer, 2, most, LANES), f32),
            pltpu.VMEM((chunks, outer, rows, LANES), f32),
            pltpu.VMEM((chunks, 2, outer, rows, LANES), f32),
            pltpu.VMEM((chunks, rows, LANES), f32),
            pltpu.VMEM((chunks, outer, 2, 2, rows, LANES), f32),
            pltpu.VMEM((len(Z_FIRST), outer, 2, 2, most, LANES), f32),
            pltpu.VMEM((len(Z_FIRST), 2, 2, most, LANES), f32),
            pltpu.VMEM((len(Z_FIRST), 2, most, LANES), f32),
            pltpu.VMEM((2, 6 + outer, 8, LANES), f32),
            pltpu.VMEM((2, levels, LANES), f32),
            pltpu.VMEM((8, LANES), f32),
            pltpu.VMEM((8, LANES), f32),
            pltpu.VMEM((modes, columns), f32),
            dma((2, BLOCKS)), dma((3,)),
            dma((2 * chunks, 4)), dma((2 * chunks, 4)),
            dma((2 * chunks, outer)), dma((2 * chunks, 2, outer)),
            dma((2 * chunks, outer)), dma((2 * chunks, outer)),
            dma((2, 6 + outer)), dma((2, 6 + outer)),
            dma((1,)), dma((1,)),
        ],
        compiler_params=pltpu.CompilerParams(
            collective_id=0, has_side_effects=True, vmem_limit_bytes=limit
        ),
        name="covariance",
    )(*(
        pltpu.with_memory_space_constraint(array, pltpu.HBM)
        for array in (perturbations, gradient, horizontal, area.reshape(1, columns), vertical.T)
    ))
    return increment, background[0, :vectors]


def solution(mesh):
    return jax.shard_map(
        per_device,
        mesh=mesh,
        in_specs=(
            P(None, "lev", "col"),
            P(None, "lev", "col"),
            P(None, "col"),
            P("col"),
            P(None, "lev"),
        ),
        out_specs=(P(None, "lev", "col"), P()),
        check_vma=False,
    )
```

```python
import functools

import jax
import jax.numpy as jnp
from jax import lax
from jax.experimental import pallas as pl
from jax.experimental.pallas import tpu as pltpu
from jax.sharding import PartitionSpec as P

LANES = 128
NT = (((1,), (1,)), ((), ()))
TN = (((0,), (0,)), ((), ()))
NN = (((1,), (0,)), ((), ()))
UNROLL = 8
BLOCKS = 2
OUT_BLOCKS = 2
Z_FIRST = (0, 4)


def split(x):
    high = x.astype(jnp.bfloat16)
    low = (x - high.astype(jnp.float32)).astype(jnp.bfloat16)
    return high, low


def exact_dot(a, b, dims):
    return lax.dot_general(
        a, b, dims, precision=lax.Precision.HIGHEST, preferred_element_type=jnp.float32
    )


PLAN = (
    0, 800, 101, 100, 3, 107, 106, 4, 109, 108, 2, 104, 201, 105,
    1, 207, 206, 103, 209, 208, 200, 301, 900, 205, 306, 102, 307, 309,
    300, 203, 1000, 305, 204, 308, 1300, 401, 202, 1800, 406, 400, 303, 407,
    304, 500, 302, 408, 1100, 409, 1804, 501, 506, 404, 1200, 600, 403, 405,
    504, 507, 402, 601, 606, 1900, 604, 509, 508, 1400, 1501, 607, 503, 502,
    505, 608, 1904, 1001, 609, 603, 605, 602, 1101, 703, 1201, 704, 700, 701,
    702, 1600, 1701,
)


def order(chunks, stages):
    if chunks == 5:
        entries = [(entry // 100, entry % 100) for entry in PLAN]
    else:
        starts = (0, 5, 10, 16, 22, 28, 34, 40)
        timed = [(start + 2.8 * j, k, j) for k, start in enumerate(starts) if k in (0, 7) for j in range(chunks)]
        timed += [
            (start + 1.4 * i, k, i)
            for k, start in enumerate(starts) if k not in (0, 7) for i in range(2 * chunks)
        ]
        timed += [(start + 1.4 * i, k, i) for k, start in ((18, 19), (19, 37)) for i in Z_FIRST]
        late = 22 + 2.8 * chunks
        timed += [
            (4.9, 8, 0), (4.95, 9, 0), (12, 10, 0), (16, 11, 0), (18, 12, 0), (21, 13, 0),
            (late, 14, 0), (late + 1, 15, 1), (late + 4, 10, 1), (late + 7, 11, 1),
            (late + 9, 12, 1), (1e6, 16, 0), (2e6, 17, 1),
        ]
        entries = [entry[1:] for entry in sorted(timed)]
    return [(stages[k], i) for k, i in entries]


def kernel(
    sizes, n, pert_hbm, grad_hbm, hor_hbm, area_hbm, vert_hbm, acc, bg_ref,
    pert_ref, grad_ref, hor_ref, area_ref, vert_ref,
    halves, weighted, terms, first, second, third, raised, lifted,
    z_in, z_sum, plane, totals, verticals, sums, weights, scaled,
    load_p, load_s, send_h, recv_h, send_g, recv_g, send_l, recv_l,
    send_t, recv_t, send_v, recv_v,
):
    members, levels, vectors, modes, columns = sizes
    group = LANES // vectors
    chunks = modes // group
    vmodes = vert_ref.shape[1]
    rows = terms.shape[4]
    tiles = rows // levels
    outer = n // 4
    used = members * levels
    apart = -(-members // LANES) * LANES
    me = lax.axis_index("col")
    lev = lax.axis_index("lev")
    other = 1 - lev
    x = lax.rem(me, 2)
    y = lax.rem(lax.div(me, 2), 2)
    h = lax.div(me, 4)
    not_x, not_y = 1 - x, 1 - y
    x_peer = (4 * h + 2 * y + not_x, lev)
    y_peer = (4 * h + 2 * not_y + x, lev)
    partner = (me, other)
    mesh_id = pl.DeviceIdType.MESH
    barrier = pltpu.get_barrier_semaphore()

    def along(p):
        return 4 * lax.rem(h + p, outer) + 2 * y + x

    def greet(device):
        pl.semaphore_signal(barrier, inc=1, device_id=device, device_id_type=mesh_id)

    def greet_outer(p, carry):
        greet((along(p), lev))
        greet((along(p), other))
        return carry

    for device in (x_peer, y_peer, partner):
        greet(device)
    lax.fori_loop(1, outer, greet_outer, 0)

    wide_block = columns // BLOCKS

    def load_block(q):
        part = pl.ds(q * wide_block, wide_block)
        return (
            pltpu.make_async_copy(
                pert_hbm.at[:, :, part], pert_ref.at[:, :, part], load_p.at[0, q]
            ),
            pltpu.make_async_copy(
                grad_hbm.at[:, :, part], grad_ref.at[:, :, part], load_p.at[1, q]
            ),
        )

    small = [
        pltpu.make_async_copy(source, target, load_s.at[i])
        for i, (source, target) in enumerate(
            ((area_hbm, area_ref), (hor_hbm, hor_ref), (vert_hbm, vert_ref))
        )
    ]
    for copy in small:
        copy.start()
    for q in range(BLOCKS):
        for copy in load_block(q):
            copy.start()

    def remote(src, dst, send, recv, device):
        return pltpu.make_async_remote_copy(
            src_ref=src, dst_ref=dst, send_sem=send, recv_sem=recv,
            device_id=device, device_id_type=mesh_id,
        )

    def piece(i):
        j, side = i // 2, i % 2
        count = (tiles + 1 - j % 2) // 2 * levels
        start, size = (0, count) if side == 0 else (count, rows - count)
        return j, side, pl.ds(start, size), size

    def half_copy(i, k, src, dst, device):
        return remote(src, dst, send_h.at[i, k], recv_h.at[i, k], device)

    def one(i):
        j, side, span, size = piece(i)
        target = first.at[i, :, :, pl.ds(0, size)]
        if side == 0:
            return half_copy(i, 0, terms.at[j, :, :, not_x, span], target, x_peer)
        return half_copy(i, 0, terms.at[j, :, not_y, :, span], target, y_peer)

    def two(i):
        j, side, span, size = piece(i)
        index, device = (not_y, y_peer) if side == 0 else (not_x, x_peer)
        source = first.at[i, :, index, pl.ds(0, size)]
        return half_copy(i, 1, source, second.at[j, :, span], device)

    def keeper(i):
        return i % 2

    def z_copy(i, p):
        j, side, span, size = piece(i)
        return remote(
            terms.at[j, lax.rem(h + p, outer), :, :, span],
            z_in.at[Z_FIRST.index(i), p, :, :, pl.ds(0, size)],
            send_g.at[i, p], recv_g.at[i, lev, p], (along(p), lev),
        )

    def plane_one(i):
        j, side, span, size = piece(i)
        k = Z_FIRST.index(i)
        source = z_sum.at[k, :, not_x] if side == 0 else z_sum.at[k, not_y]
        rows_ = pl.ds(0, size)
        source = source.at[:, rows_]
        target = plane.at[k, :, rows_]
        return half_copy(i, 0, source, target, x_peer if side == 0 else y_peer)

    def plane_two(i):
        j, side, span, size = piece(i)
        index, device = (not_y, y_peer) if side == 0 else (not_x, x_peer)
        source = plane.at[Z_FIRST.index(i), index, pl.ds(0, size)]
        return half_copy(i, 1, source, second.at[j, h, span], device)

    def back_one(i, yy, xx):
        j, side, span, size = piece(i)
        if side == 0:
            block = lifted.at[j, h, yy, x, span]
            return half_copy(i, 2, block, block, y_peer)
        block = lifted.at[j, h, y, xx, span]
        return half_copy(i, 2, block, block, x_peer)

    def back_two(i, yy, xx):
        j, side, span, size = piece(i)
        if side == 0:
            block = lifted.at[j, h, :, xx, span]
            return half_copy(i, 3, block, block, x_peer)
        block = lifted.at[j, h, yy, :, span]
        return half_copy(i, 3, block, block, y_peer)

    def back_z(i, p, slot):
        j, side, span, size = piece(i)
        block = lifted.at[j, slot, :, :, span]
        return remote(block, block, send_l.at[i, p], recv_l.at[i, p], (along(p), lev))

    def each_outer(step):
        def body(p, carry):
            step(p)
            return carry

        lax.fori_loop(1, outer, body, 0)

    def outer_copy(i, p, source):
        j, side, span, size = piece(i)
        return remote(
            second.at[j, lax.rem(h + p, outer), span], third.at[j, source, p, span],
            send_g.at[i, p], recv_g.at[i, source, p], (along(p), keeper(i)),
        )

    def lifted_copy(i, p, slot):
        j, side, span, size = piece(i)
        block = lifted.at[j, slot, y, x, span]
        return remote(block, block, send_l.at[i, p], recv_l.at[i, p], (along(p), lev))

    def raised_copy(i, p, slot):
        j, side, span, size = piece(i)
        return remote(
            raised.at[j, span], lifted.at[j, slot, y, x, span],
            send_g.at[i, p], recv_l.at[i, p], (along(p), other),
        )

    def three(i, yy, xx):
        j, side, span, size = piece(i)
        if side == 0:
            block = lifted.at[j, :, yy, x, span]
            return half_copy(i, 2, block, block, y_peer)
        block = lifted.at[j, :, y, xx, span]
        return half_copy(i, 2, block, block, x_peer)

    def four(i, yy, xx):
        j, side, span, size = piece(i)
        if side == 0:
            block = lifted.at[j, :, :, xx, span]
            return half_copy(i, 3, block, block, x_peer)
        block = lifted.at[j, :, yy, :, span]
        return half_copy(i, 3, block, block, y_peer)

    def vert_copy(slot):
        block = verticals.at[slot]
        return remote(block, block, send_v.at[0], recv_v.at[0], partner)

    def total_copy(k, source, target, device):
        return remote(
            totals.at[k, source], totals.at[k, target],
            send_t.at[k, target], recv_t.at[k, target], device,
        )

    def total_outer(k, p):
        return total_copy(k, 6, 6 + p, (along(p), lev))

    def total_x(k):
        return total_copy(k, 0, 1, x_peer)

    def total_y(k):
        return total_copy(k, 2, 3, y_peer)

    def total_c(k):
        return total_copy(k, 4, 5, partner)

    def send_total_x(k):
        total_x(k).start()

    def send_total_y(k):
        total_x(k).wait_recv()
        totals[k, 2] = totals[k, 0] + totals[k, 1]
        total_y(k).start()

    def send_total_c(k):
        total_y(k).wait_recv()
        totals[k, 4] = totals[k, 2] + totals[k, 3]
        total_c(k).start()

    def send_total_outer(k):
        total_c(k).wait_recv()
        totals[k, 6] = totals[k, 4] + totals[k, 5]

        def send(p, carry):
            total_outer(k, p).start()
            return carry

        lax.fori_loop(1, outer, send, 0)

    def take_total(k):
        def take(p, carry):
            total_outer(k, p).wait_recv()
            return carry + totals[k, 6 + p]

        return lax.fori_loop(1, outer, take, totals[k, 6])

    lane = lax.broadcasted_iota(jnp.int32, (modes, LANES), 1)
    row = lax.broadcasted_iota(jnp.int32, (modes, LANES), 0)
    sums[...] = jnp.zeros(sums.shape, jnp.float32)
    verticals[lev] = jnp.zeros(verticals.shape[1:], jnp.float32)
    if used < n * rows:
        for j in range(chunks):
            flat = terms.at[j].reshape(n * rows, LANES)
            flat[used:, :] = jnp.zeros((n * rows - used, LANES), jnp.float32)
    for copy in small:
        copy.wait()
    area = area_ref[...]
    verticals[lev, :, :vmodes] = vert_ref[...]

    def prepare():
        for q in range(BLOCKS):
            for copy in load_block(q):
                copy.wait()
            for c in range(q * wide_block, (q + 1) * wide_block, LANES):
                lanes = slice(c, c + LANES)
                for k in range(0, members, 16):
                    high, low = split(jnp.swapaxes(pert_ref[k : k + 16, :, lanes], 0, 1))
                    halves[:, k : k + 16, lanes] = high
                    halves[:, apart + k : apart + k + 16, lanes] = low
                for v in range(0, vectors, 8):
                    block = jnp.swapaxes(grad_ref[v : v + 8, :, lanes], 0, 1)
                    weighted[:, v : v + 8, lanes] = block * area[:, lanes]

    def statistics():
        power = jnp.sum(area * hor_ref[...] * hor_ref[...], axis=1, keepdims=True)
        powers = jnp.sum(
            jnp.where(lane == row, jnp.broadcast_to(power, (modes, LANES)), 0.0),
            axis=0, keepdims=True,
        )
        total = jnp.broadcast_to(jnp.sum(area, axis=1, keepdims=True), (1, LANES))
        stat_row = jnp.where(lane[:1] == modes, total, powers)
        totals[0, 0] = jnp.broadcast_to(stat_row, totals.shape[2:])

    def over_levels(step):
        def body(i, carry):
            for u in range(UNROLL):
                step(i * UNROLL + u)
            return carry

        lax.fori_loop(0, levels // UNROLL, body, 0)

    def adjoint(j):
        flat = terms.at[j].reshape(n * rows, LANES)

        def step(l):
            base = weighted[l]
            products = jnp.concatenate(
                [base * hor_ref[b : b + 1, :] for b in range(j * group, (j + 1) * group)],
                axis=0,
            )
            out = lax.dot_general(
                jnp.concatenate(split(products), axis=0), halves[l], NT,
                preferred_element_type=jnp.float32,
            )
            value = out[:LANES, :members] + (out[:LANES, apart:] + out[LANES:, :members])
            flat[pl.ds(l, members, stride=levels), :] = value.T

        over_levels(step)

    def send_one(i):
        if i in Z_FIRST:
            each_outer(lambda p: z_copy(i, p).start())
        else:
            one(i).start()

    def send_two(i):
        j, side, span, size = piece(i)
        if i in Z_FIRST:
            k = Z_FIRST.index(i)
            z_sum[k, :, :, :size] = terms[j, h, :, :, span]

            def take(p):
                z_copy(i, p).wait_recv()
                z_sum[k, :, :, :size] += z_in[k, p, :, :, :size]

            each_outer(take)
            plane_one(i).start()
            return
        one(i).wait_recv()

        def add(q, carry):
            if side == 0:
                first[i, q, not_y, :size] += terms[j, q, not_y, x, span]
            else:
                first[i, q, not_x, :size] += terms[j, q, y, not_x, span]
            return carry

        lax.fori_loop(0, outer, add, 0)
        two(i).start()

    def send_three(i):
        j, side, span, size = piece(i)
        if i in Z_FIRST:
            k = Z_FIRST.index(i)
            plane_one(i).wait_recv()
            if side == 0:
                plane[k, not_y, :size] += z_sum[k, not_y, x, :size]
            else:
                plane[k, not_x, :size] += z_sum[k, y, not_x, :size]
            plane_two(i).start()
            return
        two(i).wait_recv()

        def add_second(there):
            mine = first[i, there, y if side == 0 else x, :size]
            second[j, there, span] += terms[j, there, y, x, span] + mine

        def send_outer(p, carry):
            add_second(lax.rem(h + p, outer))
            outer_copy(i, p, lev).start()
            return carry

        lax.fori_loop(1, outer, send_outer, 0)
        add_second(h)

        @pl.when(lev != keeper(i))
        def _():
            outer_copy(i, 0, lev).start()

    def z_own(i):
        j, side, span, size = piece(i)
        k = Z_FIRST.index(i)
        plane_two(i).wait_recv()
        second[j, h, span] += z_sum[k, y, x, :size] + plane[k, y if side == 0 else x, :size]

        @pl.when(lev != keeper(i))
        def _():
            outer_copy(i, 0, lev).start()

    def mix(i):
        j, side, span, size = piece(i)

        @pl.when(lev == keeper(i))
        def _():
            def take(p, carry):
                outer_copy(i, p, lev).wait_send()
                outer_copy(i, p, lev).wait_recv()
                second[j, h, span] += third[j, lev, p, span]
                outer_copy(i, p, other).wait_recv()
                third[j, other, 0, span] += third[j, other, p, span]
                return carry

            outer_copy(i, 0, other).wait_recv()
            if i not in Z_FIRST:
                lax.fori_loop(1, outer, take, 0)

            def wide(block):
                return jnp.concatenate(
                    [block[t : t + levels] for t in range(0, size, levels)], axis=1
                )

            far = verticals[other][:, :vmodes]
            control = exact_dot(vert_ref[...], wide(second[j, h, span]), TN) + exact_dot(
                far, wide(third[j, other, 0, span]), TN
            )
            near_lifted = exact_dot(vert_ref[...], control, NN)
            far_lifted = exact_dot(far, control, NN)
            square = jnp.zeros((1, LANES), jnp.float32)
            for t in range(size // levels):
                lanes = slice(t * LANES, (t + 1) * LANES)
                part = pl.ds(span.start + t * levels, levels)
                lifted[j, h, y, x, part, :] = near_lifted[:, lanes]
                raised[j, part, :] = far_lifted[:, lanes]
                square = square + jnp.sum(
                    control[:, lanes] * control[:, lanes], axis=0, keepdims=True
                )
            sums[j : j + 1, :] = sums[j : j + 1, :] + square

            def start_lifted(p, carry):
                lifted_copy(i, p, h).start()
                raised_copy(i, p, h).start()
                return carry

            raised_copy(i, 0, h).start()
            if i not in Z_FIRST:
                lax.fori_loop(1, outer, start_lifted, 0)

    def send_g2(i):
        if i in Z_FIRST:
            @pl.when(lev != keeper(i))
            def _():
                raised_copy(i, 0, h).wait_recv()

            back_one(i, y, x).start()
            return

        @pl.when(lev == keeper(i))
        def _():
            def take(p, carry):
                lifted_copy(i, p, lax.rem(h + outer - p, outer)).wait_recv()
                return carry

            lax.fori_loop(1, outer, take, 0)

        @pl.when(lev != keeper(i))
        def _():
            def take(p, carry):
                raised_copy(i, p, lax.rem(h + outer - p, outer)).wait_recv()
                return carry

            lax.fori_loop(0, outer, take, 0)

        three(i, y, x).start()

    def send_g3(i):
        if i in Z_FIRST:
            back_one(i, not_y, not_x).wait_recv()
            back_two(i, y, x).start()
        else:
            three(i, not_y, not_x).wait_recv()
            four(i, y, x).start()

    def send_g4(i):
        back_two(i, not_y, not_x).wait_recv()
        each_outer(lambda p: back_z(i, p, h).start())

    started = []

    def forward(j):
        fresh = not started
        started.append(j)
        for i in (2 * j, 2 * j + 1):
            if i in Z_FIRST:
                each_outer(lambda p: back_z(i, p, lax.rem(h + outer - p, outer)).wait_recv())
            else:
                four(i, not_y, not_x).wait_recv()
        flat = lifted.at[j].reshape(n * rows, LANES)
        width = 256

        def step(l):
            high, low = split(flat[pl.ds(l, members, stride=levels), :])
            lhs = jnp.concatenate([high, high, low], axis=0)
            for c in range(0, columns, width):
                cols = slice(c, c + width)
                top = halves[l, :members, cols]
                rhs = jnp.concatenate([top, halves[l, apart:, cols], top], axis=0)
                spread = lax.dot_general(lhs, rhs, TN, preferred_element_type=jnp.float32)
                value = None if fresh else acc[l, :, cols]
                for g in range(group):
                    b = j * group + g
                    term = spread[g * vectors : (g + 1) * vectors] * scaled[b : b + 1, cols]
                    value = term if value is None else value + term
                acc[l, :, cols] = value

        over_levels(step)

    def take_stats(k):
        stat = 0.5 * take_total(k)
        spread = jnp.broadcast_to(stat[:1], (modes, LANES))
        power = jnp.sum(jnp.where(lane == row, spread, 0.0), axis=1, keepdims=True)
        whole = jnp.sum(jnp.where(lane == modes, spread, 0.0), axis=1, keepdims=True)
        factor = 1.0 / jnp.sqrt(modes * (power / whole + 1e-06))
        scale = factor * (columns * n / whole)
        scaled[...] = hor_ref[...] * (factor * scale)
        placed = jnp.where(
            lax.div(lane, vectors) == lax.rem(row, group),
            jnp.broadcast_to(scale, lane.shape), 0.0,
        )
        for j in range(chunks):
            weights[j : j + 1, :] = jnp.sum(
                placed[j * group : (j + 1) * group], axis=0, keepdims=True
            )

    def gather_sums(k):
        part = jnp.zeros((1, LANES), jnp.float32)
        for j in range(chunks):
            weight = weights[j : j + 1, :]
            part = part + sums[j : j + 1, :] * weight * weight
        totals[k, 0] = jnp.broadcast_to(part, totals.shape[2:])
        send_total_x(k)

    def finish_sums(k):
        part = take_total(k)
        folded = part
        for g in range(1, group):
            folded = folded + pltpu.roll(part, g * vectors, 1)
        bg_ref[...] = 0.5 * folded

    def meet(k):
        pl.semaphore_wait(barrier, 3 + 2 * (outer - 1))
        vert_copy(lev).start()

    def take_vert(k):
        vert_copy(other).wait_recv()

    def set_stats(k):
        statistics()
        send_total_x(k)

    def finish_out(k):
        pass

    prepare()
    for stage, i in order(chunks, (
        adjoint, send_one, send_two, send_three, mix, send_g2, send_g3, forward, meet, set_stats,
        send_total_y, send_total_c, send_total_outer, take_vert, take_stats, gather_sums,
        finish_out, finish_sums, z_own, send_g4,
    )):
        stage(i)

    for i in range(2 * chunks):
        if i in Z_FIRST:
            for copy in (plane_one(i), plane_two(i), back_one(i, y, x), back_two(i, y, x)):
                copy.wait_send()
            each_outer(lambda p: z_copy(i, p).wait_send())
            each_outer(lambda p: back_z(i, p, h).wait_send())

            @pl.when(lev != keeper(i))
            def _():
                outer_copy(i, 0, lev).wait_send()

            @pl.when(lev == keeper(i))
            def _():
                raised_copy(i, 0, h).wait_send()

            continue
        for copy in (one(i), two(i), three(i, y, x), four(i, y, x)):
            copy.wait_send()

        @pl.when(lev != keeper(i))
        def _():
            def sent(p, carry):
                outer_copy(i, p, lev).wait_send()
                return carry

            lax.fori_loop(0, outer, sent, 0)

        @pl.when(lev == keeper(i))
        def _():
            def sent(p, carry):
                lifted_copy(i, p, h).wait_send()
                raised_copy(i, p, h).wait_send()
                return carry

            raised_copy(i, 0, h).wait_send()
            lax.fori_loop(1, outer, sent, 0)

    for k in range(2):
        for copy in (total_x(k), total_y(k), total_c(k)):
            copy.wait_send()

        def sent_total(p, carry):
            total_outer(k, p).wait_send()
            return carry

        lax.fori_loop(1, outer, sent_total, 0)
    vert_copy(lev).wait_send()


def output_kernel(acc_ref, halved_ref, out_ref, bg_ref):
    vectors, levels, width = out_ref.shape
    bg_ref[...] = halved_ref[:1, :vectors]
    for c in range(0, width, LANES):
        lanes = slice(c, c + LANES)
        for v in range(0, vectors, 8):
            out_ref[v : v + 8, :, lanes] = jnp.swapaxes(acc_ref[:, v : v + 8, lanes], 0, 1)


def per_device(perturbations, gradient, horizontal, area, vertical):
    members, levels, columns = perturbations.shape
    vectors = gradient.shape[0]
    modes = horizontal.shape[0]
    n = lax.axis_size("col")
    sizes = (members, levels, vectors, modes, columns)
    chunks = modes * vectors // LANES
    tiles = max(2, -(-members // n))
    rows = tiles * levels
    outer = n // 4
    apart = -(-members // LANES) * LANES
    most = (tiles + 1) // 2 * levels
    f32 = jnp.float32
    vmem = pl.BlockSpec(memory_space=pltpu.VMEM)
    dma = pltpu.SemaphoreType.DMA

    held = chunks * n * rows * LANES * 4 * 9 // 2
    limit = min(60 * 2**20, held + 20 * 2**20)
    by_level, halved = pl.pallas_call(
        functools.partial(kernel, sizes, n),
        out_shape=(
            jax.ShapeDtypeStruct((levels, vectors, columns), f32),
            jax.ShapeDtypeStruct((8, LANES), f32),
        ),
        in_specs=[pl.BlockSpec(memory_space=pltpu.HBM)] * 5,
        out_specs=(vmem, vmem),
        scratch_shapes=[
            pltpu.VMEM((members, levels, columns), f32),
            pltpu.VMEM((vectors, levels, columns), f32),
            pltpu.VMEM((modes, columns), f32),
            pltpu.VMEM((1, columns), f32),
            pltpu.VMEM((levels, vertical.shape[0]), f32),
            pltpu.VMEM((levels, apart + members, columns), jnp.bfloat16),
            pltpu.VMEM((levels, vectors, columns), f32),
            pltpu.VMEM((chunks, outer, 2, 2, rows, LANES), f32),
            pltpu.VMEM((2 * chunks, outer, 2, most, LANES), f32),
            pltpu.VMEM((chunks, outer, rows, LANES), f32),
            pltpu.VMEM((chunks, 2, outer, rows, LANES), f32),
            pltpu.VMEM((chunks, rows, LANES), f32),
            pltpu.VMEM((chunks, outer, 2, 2, rows, LANES), f32),
            pltpu.VMEM((len(Z_FIRST), outer, 2, 2, most, LANES), f32),
            pltpu.VMEM((len(Z_FIRST), 2, 2, most, LANES), f32),
            pltpu.VMEM((len(Z_FIRST), 2, most, LANES), f32),
            pltpu.VMEM((2, 6 + outer, 8, LANES), f32),
            pltpu.VMEM((2, levels, LANES), f32),
            pltpu.VMEM((8, LANES), f32),
            pltpu.VMEM((8, LANES), f32),
            pltpu.VMEM((modes, columns), f32),
            dma((2, BLOCKS)), dma((3,)),
            dma((2 * chunks, 4)), dma((2 * chunks, 4)),
            dma((2 * chunks, outer)), dma((2 * chunks, 2, outer)),
            dma((2 * chunks, outer)), dma((2 * chunks, outer)),
            dma((2, 6 + outer)), dma((2, 6 + outer)),
            dma((1,)), dma((1,)),
        ],
        compiler_params=pltpu.CompilerParams(
            collective_id=0, has_side_effects=True, vmem_limit_bytes=limit
        ),
        name="covariance",
    )(*(
        pltpu.with_memory_space_constraint(array, pltpu.HBM)
        for array in (perturbations, gradient, horizontal, area.reshape(1, columns), vertical.T)
    ))
    width = columns // OUT_BLOCKS
    increment, background = pl.pallas_call(
        output_kernel,
        grid=(OUT_BLOCKS,),
        out_shape=(
            jax.ShapeDtypeStruct((vectors, levels, columns), f32),
            jax.ShapeDtypeStruct((1, vectors), f32),
        ),
        in_specs=[
            pl.BlockSpec((levels, vectors, width), lambda c: (0, 0, c)),
            pl.BlockSpec((8, LANES), lambda c: (0, 0)),
        ],
        out_specs=(
            pl.BlockSpec((vectors, levels, width), lambda c: (0, 0, c)),
            pl.BlockSpec((1, vectors), lambda c: (0, 0)),
        ),
        compiler_params=pltpu.CompilerParams(vmem_limit_bytes=8 * 2**20),
        name="output",
    )(by_level, halved)
    return increment, background.reshape(vectors)


def solution(mesh):
    return jax.shard_map(
        per_device,
        mesh=mesh,
        in_specs=(
            P(None, "lev", "col"),
            P(None, "lev", "col"),
            P(None, "col"),
            P("col"),
            P(None, "lev"),
        ),
        out_specs=(P(None, "lev", "col"), P()),
        check_vma=False,
    )
```

```python
import functools

import jax
import jax.numpy as jnp
from jax import lax
from jax.experimental import pallas as pl
from jax.experimental.pallas import tpu as pltpu
from jax.sharding import PartitionSpec as P

LANES = 128
NT = (((1,), (1,)), ((), ()))
TN = (((0,), (0,)), ((), ()))
NN = (((1,), (0,)), ((), ()))
UNROLL = 8
BLOCKS = 2
OUT_BLOCKS = 2
Z_FIRST = (0, 4)


def split(x):
    high = x.astype(jnp.bfloat16)
    low = (x - high.astype(jnp.float32)).astype(jnp.bfloat16)
    return high, low


def exact_dot(a, b, dims):
    return lax.dot_general(
        a, b, dims, precision=lax.Precision.HIGHEST, preferred_element_type=jnp.float32
    )


PLAN = (
    2, 800, 104, 105, 3, 106, 107, 4, 108, 109, 0, 100, 205, 1,
    103, 207, 209, 208, 204, 206, 101, 305, 900, 102, 307, 203, 309, 304,
    308, 306, 200, 202, 1000, 1300, 405, 201, 303, 1804, 407, 404, 300, 302,
    1100, 504, 301, 408, 505, 1200, 409, 1800, 403, 604, 400, 507, 406, 500,
    605, 402, 401, 508, 1400, 1904, 607, 1501, 600, 509, 503, 506, 608, 502,
    1900, 1001, 501, 609, 603, 606, 1101, 602, 1201, 601, 702, 704, 703, 701,
    700, 1600, 1701,
)


def order(chunks, stages):
    if chunks == 5:
        entries = [(entry // 100, entry % 100) for entry in PLAN]
    else:
        starts = (0, 5, 10, 16, 22, 28, 34, 40)
        timed = [(start + 2.8 * j, k, j) for k, start in enumerate(starts) if k in (0, 7) for j in range(chunks)]
        timed += [
            (start + 1.4 * i, k, i)
            for k, start in enumerate(starts) if k not in (0, 7) for i in range(2 * chunks)
        ]
        timed += [(start + 1.4 * i, k, i) for k, start in ((18, 19), (19, 37)) for i in Z_FIRST]
        late = 22 + 2.8 * chunks
        timed += [
            (4.9, 8, 0), (4.95, 9, 0), (12, 10, 0), (16, 11, 0), (18, 12, 0), (21, 13, 0),
            (late, 14, 0), (late + 1, 15, 1), (late + 4, 10, 1), (late + 7, 11, 1),
            (late + 9, 12, 1), (1e6, 16, 0), (2e6, 17, 1),
        ]
        entries = [entry[1:] for entry in sorted(timed)]
    return [(stages[k], i) for k, i in entries]


def kernel(
    sizes, n, pert_hbm, grad_hbm, hor_hbm, area_hbm, vert_hbm, acc, bg_ref,
    pert_ref, grad_ref, hor_ref, area_ref, vert_ref,
    halves, weighted, terms, first, second, third, raised, lifted,
    z_in, z_sum, plane, totals, verticals, sums, weights, scaled,
    load_p, load_s, send_h, recv_h, send_g, recv_g, send_l, recv_l,
    send_t, recv_t, send_v, recv_v,
):
    members, levels, vectors, modes, columns = sizes
    group = LANES // vectors
    chunks = modes // group
    vmodes = vert_ref.shape[1]
    rows = terms.shape[4]
    tiles = rows // levels
    outer = n // 4
    used = members * levels
    apart = -(-members // LANES) * LANES
    me = lax.axis_index("col")
    lev = lax.axis_index("lev")
    other = 1 - lev
    x = lax.rem(me, 2)
    y = lax.rem(lax.div(me, 2), 2)
    h = lax.div(me, 4)
    not_x, not_y = 1 - x, 1 - y
    x_peer = (4 * h + 2 * y + not_x, lev)
    y_peer = (4 * h + 2 * not_y + x, lev)
    partner = (me, other)
    mesh_id = pl.DeviceIdType.MESH
    barrier = pltpu.get_barrier_semaphore()

    def along(p):
        return 4 * lax.rem(h + p, outer) + 2 * y + x

    def greet(device):
        pl.semaphore_signal(barrier, inc=1, device_id=device, device_id_type=mesh_id)

    def greet_outer(p, carry):
        greet((along(p), lev))
        greet((along(p), other))
        return carry

    for device in (x_peer, y_peer, partner):
        greet(device)
    lax.fori_loop(1, outer, greet_outer, 0)

    wide_block = columns // BLOCKS

    def load_block(q):
        part = pl.ds(q * wide_block, wide_block)
        return (
            pltpu.make_async_copy(
                pert_hbm.at[:, :, part], pert_ref.at[:, :, part], load_p.at[0, q]
            ),
            pltpu.make_async_copy(
                grad_hbm.at[:, :, part], grad_ref.at[:, :, part], load_p.at[1, q]
            ),
        )

    small = [
        pltpu.make_async_copy(source, target, load_s.at[i])
        for i, (source, target) in enumerate(
            ((area_hbm, area_ref), (hor_hbm, hor_ref), (vert_hbm, vert_ref))
        )
    ]
    for copy in small:
        copy.start()
    for q in range(BLOCKS):
        for copy in load_block(q):
            copy.start()

    def remote(src, dst, send, recv, device):
        return pltpu.make_async_remote_copy(
            src_ref=src, dst_ref=dst, send_sem=send, recv_sem=recv,
            device_id=device, device_id_type=mesh_id,
        )

    def piece(i):
        j, side = i // 2, i % 2
        count = (tiles + 1 - j % 2) // 2 * levels
        start, size = (0, count) if side == 0 else (count, rows - count)
        return j, side, pl.ds(start, size), size

    def half_copy(i, k, src, dst, device):
        return remote(src, dst, send_h.at[i, k], recv_h.at[i, k], device)

    def one(i):
        j, side, span, size = piece(i)
        target = first.at[i, :, :, pl.ds(0, size)]
        if side == 0:
            return half_copy(i, 0, terms.at[j, :, :, not_x, span], target, x_peer)
        return half_copy(i, 0, terms.at[j, :, not_y, :, span], target, y_peer)

    def two(i):
        j, side, span, size = piece(i)
        index, device = (not_y, y_peer) if side == 0 else (not_x, x_peer)
        source = first.at[i, :, index, pl.ds(0, size)]
        return half_copy(i, 1, source, second.at[j, :, span], device)

    def keeper(i):
        return i % 2

    def z_copy(i, p):
        j, side, span, size = piece(i)
        return remote(
            terms.at[j, lax.rem(h + p, outer), :, :, span],
            z_in.at[Z_FIRST.index(i), p, :, :, pl.ds(0, size)],
            send_g.at[i, p], recv_g.at[i, lev, p], (along(p), lev),
        )

    def plane_one(i):
        j, side, span, size = piece(i)
        k = Z_FIRST.index(i)
        source = z_sum.at[k, :, not_x] if side == 0 else z_sum.at[k, not_y]
        rows_ = pl.ds(0, size)
        source = source.at[:, rows_]
        target = plane.at[k, :, rows_]
        return half_copy(i, 0, source, target, x_peer if side == 0 else y_peer)

    def plane_two(i):
        j, side, span, size = piece(i)
        index, device = (not_y, y_peer) if side == 0 else (not_x, x_peer)
        source = plane.at[Z_FIRST.index(i), index, pl.ds(0, size)]
        return half_copy(i, 1, source, second.at[j, h, span], device)

    def back_one(i, yy, xx):
        j, side, span, size = piece(i)
        if side == 0:
            block = lifted.at[j, h, yy, x, span]
            return half_copy(i, 2, block, block, y_peer)
        block = lifted.at[j, h, y, xx, span]
        return half_copy(i, 2, block, block, x_peer)

    def back_two(i, yy, xx):
        j, side, span, size = piece(i)
        if side == 0:
            block = lifted.at[j, h, :, xx, span]
            return half_copy(i, 3, block, block, x_peer)
        block = lifted.at[j, h, yy, :, span]
        return half_copy(i, 3, block, block, y_peer)

    def back_z(i, p, slot):
        j, side, span, size = piece(i)
        block = lifted.at[j, slot, :, :, span]
        return remote(block, block, send_l.at[i, p], recv_l.at[i, p], (along(p), lev))

    def each_outer(step):
        def body(p, carry):
            step(p)
            return carry

        lax.fori_loop(1, outer, body, 0)

    def outer_copy(i, p, source):
        j, side, span, size = piece(i)
        return remote(
            second.at[j, lax.rem(h + p, outer), span], third.at[j, source, p, span],
            send_g.at[i, p], recv_g.at[i, source, p], (along(p), keeper(i)),
        )

    def lifted_copy(i, p, slot):
        j, side, span, size = piece(i)
        block = lifted.at[j, slot, y, x, span]
        return remote(block, block, send_l.at[i, p], recv_l.at[i, p], (along(p), lev))

    def raised_copy(i, p, slot):
        j, side, span, size = piece(i)
        return remote(
            raised.at[j, span], lifted.at[j, slot, y, x, span],
            send_g.at[i, p], recv_l.at[i, p], (along(p), other),
        )

    def three(i, yy, xx):
        j, side, span, size = piece(i)
        if side == 0:
            block = lifted.at[j, :, yy, x, span]
            return half_copy(i, 2, block, block, y_peer)
        block = lifted.at[j, :, y, xx, span]
        return half_copy(i, 2, block, block, x_peer)

    def four(i, yy, xx):
        j, side, span, size = piece(i)
        if side == 0:
            block = lifted.at[j, :, :, xx, span]
            return half_copy(i, 3, block, block, x_peer)
        block = lifted.at[j, :, yy, :, span]
        return half_copy(i, 3, block, block, y_peer)

    def vert_copy(slot):
        block = verticals.at[slot]
        return remote(block, block, send_v.at[0], recv_v.at[0], partner)

    def total_copy(k, source, target, device):
        return remote(
            totals.at[k, source], totals.at[k, target],
            send_t.at[k, target], recv_t.at[k, target], device,
        )

    def total_outer(k, p):
        return total_copy(k, 6, 6 + p, (along(p), lev))

    def total_x(k):
        return total_copy(k, 0, 1, x_peer)

    def total_y(k):
        return total_copy(k, 2, 3, y_peer)

    def total_c(k):
        return total_copy(k, 4, 5, partner)

    def send_total_x(k):
        total_x(k).start()

    def send_total_y(k):
        total_x(k).wait_recv()
        totals[k, 2] = totals[k, 0] + totals[k, 1]
        total_y(k).start()

    def send_total_c(k):
        total_y(k).wait_recv()
        totals[k, 4] = totals[k, 2] + totals[k, 3]
        total_c(k).start()

    def send_total_outer(k):
        total_c(k).wait_recv()
        totals[k, 6] = totals[k, 4] + totals[k, 5]

        def send(p, carry):
            total_outer(k, p).start()
            return carry

        lax.fori_loop(1, outer, send, 0)

    def take_total(k):
        def take(p, carry):
            total_outer(k, p).wait_recv()
            return carry + totals[k, 6 + p]

        return lax.fori_loop(1, outer, take, totals[k, 6])

    lane = lax.broadcasted_iota(jnp.int32, (modes, LANES), 1)
    row = lax.broadcasted_iota(jnp.int32, (modes, LANES), 0)
    sums[...] = jnp.zeros(sums.shape, jnp.float32)
    verticals[lev] = jnp.zeros(verticals.shape[1:], jnp.float32)
    if used < n * rows:
        for j in range(chunks):
            flat = terms.at[j].reshape(n * rows, LANES)
            flat[used:, :] = jnp.zeros((n * rows - used, LANES), jnp.float32)
    for copy in small:
        copy.wait()
    area = area_ref[...]
    verticals[lev, :, :vmodes] = vert_ref[...]

    def prepare():
        for q in range(BLOCKS):
            for copy in load_block(q):
                copy.wait()
            for c in range(q * wide_block, (q + 1) * wide_block, LANES):
                lanes = slice(c, c + LANES)
                for k in range(0, members, 16):
                    high, low = split(jnp.swapaxes(pert_ref[k : k + 16, :, lanes], 0, 1))
                    halves[:, k : k + 16, lanes] = high
                    halves[:, apart + k : apart + k + 16, lanes] = low
                for v in range(0, vectors, 8):
                    block = jnp.swapaxes(grad_ref[v : v + 8, :, lanes], 0, 1)
                    weighted[:, v : v + 8, lanes] = block * area[:, lanes]

    def statistics():
        power = jnp.sum(area * hor_ref[...] * hor_ref[...], axis=1, keepdims=True)
        powers = jnp.sum(
            jnp.where(lane == row, jnp.broadcast_to(power, (modes, LANES)), 0.0),
            axis=0, keepdims=True,
        )
        total = jnp.broadcast_to(jnp.sum(area, axis=1, keepdims=True), (1, LANES))
        stat_row = jnp.where(lane[:1] == modes, total, powers)
        totals[0, 0] = jnp.broadcast_to(stat_row, totals.shape[2:])

    def over_levels(step):
        def body(i, carry):
            for u in range(UNROLL):
                step(i * UNROLL + u)
            return carry

        lax.fori_loop(0, levels // UNROLL, body, 0)

    def adjoint(j):
        flat = terms.at[j].reshape(n * rows, LANES)

        def step(l):
            base = weighted[l]
            products = jnp.concatenate(
                [base * hor_ref[b : b + 1, :] for b in range(j * group, (j + 1) * group)],
                axis=0,
            )
            out = lax.dot_general(
                jnp.concatenate(split(products), axis=0), halves[l], NT,
                preferred_element_type=jnp.float32,
            )
            value = out[:LANES, :members] + (out[:LANES, apart:] + out[LANES:, :members])
            flat[pl.ds(l, members, stride=levels), :] = value.T

        over_levels(step)

    def send_one(i):
        if i in Z_FIRST:
            each_outer(lambda p: z_copy(i, p).start())
        else:
            one(i).start()

    def send_two(i):
        j, side, span, size = piece(i)
        if i in Z_FIRST:
            k = Z_FIRST.index(i)
            z_sum[k, :, :, :size] = terms[j, h, :, :, span]

            def take(p):
                z_copy(i, p).wait_recv()
                z_sum[k, :, :, :size] += z_in[k, p, :, :, :size]

            each_outer(take)
            plane_one(i).start()
            return
        one(i).wait_recv()

        def add(q, carry):
            if side == 0:
                first[i, q, not_y, :size] += terms[j, q, not_y, x, span]
            else:
                first[i, q, not_x, :size] += terms[j, q, y, not_x, span]
            return carry

        lax.fori_loop(0, outer, add, 0)
        two(i).start()

    def send_three(i):
        j, side, span, size = piece(i)
        if i in Z_FIRST:
            k = Z_FIRST.index(i)
            plane_one(i).wait_recv()
            if side == 0:
                plane[k, not_y, :size] += z_sum[k, not_y, x, :size]
            else:
                plane[k, not_x, :size] += z_sum[k, y, not_x, :size]
            plane_two(i).start()
            return
        two(i).wait_recv()

        def add_second(there):
            mine = first[i, there, y if side == 0 else x, :size]
            second[j, there, span] += terms[j, there, y, x, span] + mine

        def send_outer(p, carry):
            add_second(lax.rem(h + p, outer))
            outer_copy(i, p, lev).start()
            return carry

        lax.fori_loop(1, outer, send_outer, 0)
        add_second(h)

        @pl.when(lev != keeper(i))
        def _():
            outer_copy(i, 0, lev).start()

    def z_own(i):
        j, side, span, size = piece(i)
        k = Z_FIRST.index(i)
        plane_two(i).wait_recv()
        second[j, h, span] += z_sum[k, y, x, :size] + plane[k, y if side == 0 else x, :size]

        @pl.when(lev != keeper(i))
        def _():
            outer_copy(i, 0, lev).start()

    def mix(i):
        j, side, span, size = piece(i)

        @pl.when(lev == keeper(i))
        def _():
            def take(p, carry):
                outer_copy(i, p, lev).wait_send()
                outer_copy(i, p, lev).wait_recv()
                second[j, h, span] += third[j, lev, p, span]
                outer_copy(i, p, other).wait_recv()
                third[j, other, 0, span] += third[j, other, p, span]
                return carry

            outer_copy(i, 0, other).wait_recv()
            if i not in Z_FIRST:
                lax.fori_loop(1, outer, take, 0)

            def wide(block):
                return jnp.concatenate(
                    [block[t : t + levels] for t in range(0, size, levels)], axis=1
                )

            far = verticals[other][:, :vmodes]
            control = exact_dot(vert_ref[...], wide(second[j, h, span]), TN) + exact_dot(
                far, wide(third[j, other, 0, span]), TN
            )
            near_lifted = exact_dot(vert_ref[...], control, NN)
            far_lifted = exact_dot(far, control, NN)
            square = jnp.zeros((1, LANES), jnp.float32)
            for t in range(size // levels):
                lanes = slice(t * LANES, (t + 1) * LANES)
                part = pl.ds(span.start + t * levels, levels)
                lifted[j, h, y, x, part, :] = near_lifted[:, lanes]
                raised[j, part, :] = far_lifted[:, lanes]
                square = square + jnp.sum(
                    control[:, lanes] * control[:, lanes], axis=0, keepdims=True
                )
            sums[j : j + 1, :] = sums[j : j + 1, :] + square

            def start_lifted(p, carry):
                lifted_copy(i, p, h).start()
                raised_copy(i, p, h).start()
                return carry

            raised_copy(i, 0, h).start()
            if i not in Z_FIRST:
                lax.fori_loop(1, outer, start_lifted, 0)

    def send_g2(i):
        if i in Z_FIRST:
            @pl.when(lev != keeper(i))
            def _():
                raised_copy(i, 0, h).wait_recv()

            back_one(i, y, x).start()
            return

        @pl.when(lev == keeper(i))
        def _():
            def take(p, carry):
                lifted_copy(i, p, lax.rem(h + outer - p, outer)).wait_recv()
                return carry

            lax.fori_loop(1, outer, take, 0)

        @pl.when(lev != keeper(i))
        def _():
            def take(p, carry):
                raised_copy(i, p, lax.rem(h + outer - p, outer)).wait_recv()
                return carry

            lax.fori_loop(0, outer, take, 0)

        three(i, y, x).start()

    def send_g3(i):
        if i in Z_FIRST:
            back_one(i, not_y, not_x).wait_recv()
            back_two(i, y, x).start()
        else:
            three(i, not_y, not_x).wait_recv()
            four(i, y, x).start()

    def send_g4(i):
        back_two(i, not_y, not_x).wait_recv()
        each_outer(lambda p: back_z(i, p, h).start())

    started = []

    def forward(j):
        fresh = not started
        started.append(j)
        for i in (2 * j, 2 * j + 1):
            if i in Z_FIRST:
                each_outer(lambda p: back_z(i, p, lax.rem(h + outer - p, outer)).wait_recv())
            else:
                four(i, not_y, not_x).wait_recv()
        flat = lifted.at[j].reshape(n * rows, LANES)
        width = 256

        def step(l):
            high, low = split(flat[pl.ds(l, members, stride=levels), :])
            lhs = jnp.concatenate([high, high, low], axis=0)
            for c in range(0, columns, width):
                cols = slice(c, c + width)
                top = halves[l, :members, cols]
                rhs = jnp.concatenate([top, halves[l, apart:, cols], top], axis=0)
                spread = lax.dot_general(lhs, rhs, TN, preferred_element_type=jnp.float32)
                value = None if fresh else acc[l, :, cols]
                for g in range(group):
                    b = j * group + g
                    term = spread[g * vectors : (g + 1) * vectors] * scaled[b : b + 1, cols]
                    value = term if value is None else value + term
                acc[l, :, cols] = value

        over_levels(step)

    def take_stats(k):
        stat = 0.5 * take_total(k)
        spread = jnp.broadcast_to(stat[:1], (modes, LANES))
        power = jnp.sum(jnp.where(lane == row, spread, 0.0), axis=1, keepdims=True)
        whole = jnp.sum(jnp.where(lane == modes, spread, 0.0), axis=1, keepdims=True)
        factor = 1.0 / jnp.sqrt(modes * (power / whole + 1e-06))
        scale = factor * (columns * n / whole)
        scaled[...] = hor_ref[...] * (factor * scale)
        placed = jnp.where(
            lax.div(lane, vectors) == lax.rem(row, group),
            jnp.broadcast_to(scale, lane.shape), 0.0,
        )
        for j in range(chunks):
            weights[j : j + 1, :] = jnp.sum(
                placed[j * group : (j + 1) * group], axis=0, keepdims=True
            )

    def gather_sums(k):
        part = jnp.zeros((1, LANES), jnp.float32)
        for j in range(chunks):
            weight = weights[j : j + 1, :]
            part = part + sums[j : j + 1, :] * weight * weight
        totals[k, 0] = jnp.broadcast_to(part, totals.shape[2:])
        send_total_x(k)

    def finish_sums(k):
        part = take_total(k)
        folded = part
        for g in range(1, group):
            folded = folded + pltpu.roll(part, g * vectors, 1)
        bg_ref[...] = 0.5 * folded

    def meet(k):
        pl.semaphore_wait(barrier, 3 + 2 * (outer - 1))
        vert_copy(lev).start()

    def take_vert(k):
        vert_copy(other).wait_recv()

    def set_stats(k):
        statistics()
        send_total_x(k)

    def finish_out(k):
        pass

    prepare()
    for stage, i in order(chunks, (
        adjoint, send_one, send_two, send_three, mix, send_g2, send_g3, forward, meet, set_stats,
        send_total_y, send_total_c, send_total_outer, take_vert, take_stats, gather_sums,
        finish_out, finish_sums, z_own, send_g4,
    )):
        stage(i)

    for i in range(2 * chunks):
        if i in Z_FIRST:
            for copy in (plane_one(i), plane_two(i), back_one(i, y, x), back_two(i, y, x)):
                copy.wait_send()
            each_outer(lambda p: z_copy(i, p).wait_send())
            each_outer(lambda p: back_z(i, p, h).wait_send())

            @pl.when(lev != keeper(i))
            def _():
                outer_copy(i, 0, lev).wait_send()

            @pl.when(lev == keeper(i))
            def _():
                raised_copy(i, 0, h).wait_send()

            continue
        for copy in (one(i), two(i), three(i, y, x), four(i, y, x)):
            copy.wait_send()

        @pl.when(lev != keeper(i))
        def _():
            def sent(p, carry):
                outer_copy(i, p, lev).wait_send()
                return carry

            lax.fori_loop(0, outer, sent, 0)

        @pl.when(lev == keeper(i))
        def _():
            def sent(p, carry):
                lifted_copy(i, p, h).wait_send()
                raised_copy(i, p, h).wait_send()
                return carry

            raised_copy(i, 0, h).wait_send()
            lax.fori_loop(1, outer, sent, 0)

    for k in range(2):
        for copy in (total_x(k), total_y(k), total_c(k)):
            copy.wait_send()

        def sent_total(p, carry):
            total_outer(k, p).wait_send()
            return carry

        lax.fori_loop(1, outer, sent_total, 0)
    vert_copy(lev).wait_send()


def output_kernel(acc_ref, halved_ref, out_ref, bg_ref):
    vectors, levels, width = out_ref.shape
    bg_ref[...] = halved_ref[:1, :vectors]
    for c in range(0, width, LANES):
        lanes = slice(c, c + LANES)
        for v in range(0, vectors, 8):
            out_ref[v : v + 8, :, lanes] = jnp.swapaxes(acc_ref[:, v : v + 8, lanes], 0, 1)


def per_device(perturbations, gradient, horizontal, area, vertical):
    members, levels, columns = perturbations.shape
    vectors = gradient.shape[0]
    modes = horizontal.shape[0]
    n = lax.axis_size("col")
    sizes = (members, levels, vectors, modes, columns)
    chunks = modes * vectors // LANES
    tiles = max(2, -(-members // n))
    rows = tiles * levels
    outer = n // 4
    apart = -(-members // LANES) * LANES
    most = (tiles + 1) // 2 * levels
    f32 = jnp.float32
    vmem = pl.BlockSpec(memory_space=pltpu.VMEM)
    dma = pltpu.SemaphoreType.DMA

    held = chunks * n * rows * LANES * 4 * 9 // 2
    limit = min(60 * 2**20, held + 20 * 2**20)
    by_level, halved = pl.pallas_call(
        functools.partial(kernel, sizes, n),
        out_shape=(
            jax.ShapeDtypeStruct((levels, vectors, columns), f32),
            jax.ShapeDtypeStruct((8, LANES), f32),
        ),
        in_specs=[pl.BlockSpec(memory_space=pltpu.HBM)] * 5,
        out_specs=(vmem, vmem),
        scratch_shapes=[
            pltpu.VMEM((members, levels, columns), f32),
            pltpu.VMEM((vectors, levels, columns), f32),
            pltpu.VMEM((modes, columns), f32),
            pltpu.VMEM((1, columns), f32),
            pltpu.VMEM((levels, vertical.shape[0]), f32),
            pltpu.VMEM((levels, apart + members, columns), jnp.bfloat16),
            pltpu.VMEM((levels, vectors, columns), f32),
            pltpu.VMEM((chunks, outer, 2, 2, rows, LANES), f32),
            pltpu.VMEM((2 * chunks, outer, 2, most, LANES), f32),
            pltpu.VMEM((chunks, outer, rows, LANES), f32),
            pltpu.VMEM((chunks, 2, outer, rows, LANES), f32),
            pltpu.VMEM((chunks, rows, LANES), f32),
            pltpu.VMEM((chunks, outer, 2, 2, rows, LANES), f32),
            pltpu.VMEM((len(Z_FIRST), outer, 2, 2, most, LANES), f32),
            pltpu.VMEM((len(Z_FIRST), 2, 2, most, LANES), f32),
            pltpu.VMEM((len(Z_FIRST), 2, most, LANES), f32),
            pltpu.VMEM((2, 6 + outer, 8, LANES), f32),
            pltpu.VMEM((2, levels, LANES), f32),
            pltpu.VMEM((8, LANES), f32),
            pltpu.VMEM((8, LANES), f32),
            pltpu.VMEM((modes, columns), f32),
            dma((2, BLOCKS)), dma((3,)),
            dma((2 * chunks, 4)), dma((2 * chunks, 4)),
            dma((2 * chunks, outer)), dma((2 * chunks, 2, outer)),
            dma((2 * chunks, outer)), dma((2 * chunks, outer)),
            dma((2, 6 + outer)), dma((2, 6 + outer)),
            dma((1,)), dma((1,)),
        ],
        compiler_params=pltpu.CompilerParams(
            collective_id=0, has_side_effects=True, vmem_limit_bytes=limit
        ),
        name="covariance",
    )(*(
        pltpu.with_memory_space_constraint(array, pltpu.HBM)
        for array in (perturbations, gradient, horizontal, area.reshape(1, columns), vertical.T)
    ))
    width = columns // OUT_BLOCKS
    increment, background = pl.pallas_call(
        output_kernel,
        grid=(OUT_BLOCKS,),
        out_shape=(
            jax.ShapeDtypeStruct((vectors, levels, columns), f32),
            jax.ShapeDtypeStruct((1, vectors), f32),
        ),
        in_specs=[
            pl.BlockSpec((levels, vectors, width), lambda c: (0, 0, c)),
            pl.BlockSpec((8, LANES), lambda c: (0, 0)),
        ],
        out_specs=(
            pl.BlockSpec((vectors, levels, width), lambda c: (0, 0, c)),
            pl.BlockSpec((1, vectors), lambda c: (0, 0)),
        ),
        compiler_params=pltpu.CompilerParams(vmem_limit_bytes=8 * 2**20),
        name="output",
    )(by_level, halved)
    return increment, background.reshape(vectors)


def solution(mesh):
    return jax.shard_map(
        per_device,
        mesh=mesh,
        in_specs=(
            P(None, "lev", "col"),
            P(None, "lev", "col"),
            P(None, "col"),
            P("col"),
            P(None, "lev"),
        ),
        out_specs=(P(None, "lev", "col"), P()),
        check_vma=False,
    )
```
